256 devices in a mesh: batch: 16 (over y, x), field: 2 (over core), dim: 8 (over z).
Axes of the slice: x: 4, y: 4, z: 8, core: 2. Of those that a mesh axis runs over, the one named last changes fastest.
Arguments:
- features: bfloat16 [26, 128, 16384], P('field', 'dim', 'batch'), may hold values from -6 to 6
- cross_weight: bfloat16 [2, 26, 128, 26, 128], P(None, 'field', 'dim'), may hold values from -0.109375 to 0.109375
- cross_bias: float32 [2, 26, 128], P(None, 'field', 'dim'), may hold values from -3 to 3
- tower_weight: bfloat16 [1024, 26, 128], P(('field', 'dim')), may hold values from -0.109375 to 0.109375
- tower_bias: float32 [1024], P(('field', 'dim')), may hold values from -3 to 3
- query_weight: bfloat16 [1024, 128], P(('field', 'dim')), may hold values from -0.1875 to 0.1875
- user_vec: bfloat16 [16384, 128], P('batch'), may hold values from -6 to 6
- candidates: bfloat16 [4096, 128], P('batch'), may hold values from -6 to 6
- positive: int32 [16384], P('batch'), may hold values from 0 to 4095
Outputs:
- crossed: bfloat16 [26, 128, 16384], P('field', 'dim', 'batch')
- losses: float32 [16384], P('batch')
The draws below stay inside these ranges and needn't reach their ends.
All inputs are finite; a program needn't handle non-finite values.
Results may differ from the reference program's by a relative error of at most 0.0049.
Values may be sent and summed in bfloat16 or wider, within the bound.
A program may use at most 64 MiB of HBM per device.

```python
import math
import jax
import jax.numpy as jnp
from jax import lax

FIELDS = 26
EMB = 128
TOWER = 1024
CROSS = 2
EX_DEV = 1024
BATCH = 16384
CANDS = 4096
N_BATCH = 16


def draw_user_vec(key, part):
    row_total = BATCH
    values = jnp.clip(jax.random.normal(jax.random.fold_in(key, 11), (row_total, EMB), jnp.float32), -6.0, 6.0)
    return values.astype(jnp.bfloat16)


def draw_candidates(key, part):
    row_total = CANDS
    values = jnp.clip(jax.random.normal(jax.random.fold_in(key, 23), (row_total, EMB), jnp.float32), -6.0, 6.0)
    return values.astype(jnp.bfloat16)


def plant(entries, rng, low, top_value):
    extent = entries.shape
    spot = [jax.random.randint(jax.random.fold_in(rng, axis), (), 0, extent[axis]) for axis in range(len(extent))]
    entries = entries.at[tuple(spot)].set(low)
    longest = extent.index(max(extent))
    spot[longest] = (spot[longest] + 1) % extent[longest]
    return entries.at[tuple(spot)].set(top_value)


def steps_of(rng, dims, split, least, largest):
    loudness = 1.0
    for dim, parts in split:
        draws = jax.random.uniform(jax.random.fold_in(jax.random.fold_in(rng, 6), dim), (parts,), jnp.float32, least / len(split), largest / len(split))
        loudness = loudness * jnp.repeat(jnp.exp(draws), dims[dim] // parts).reshape((-1,) + (1,) * (len(dims) - 1 - dim))
    return loudness


def normal_values(own_key, shape, deviation, most, cuts=(), kind=jnp.bfloat16):
    values = deviation * jax.random.normal(own_key, shape, jnp.float32)
    if cuts:
        values = values * steps_of(own_key, shape, cuts, -0.22, 0.18)
    return jnp.clip(values, -most, most).astype(kind)


def setup_inputs(seed: int = 0) -> dict:
    key_of = jax.random.split(jax.random.key(seed), 10)
    return {
        "features": normal_values(key_of[0], (FIELDS, EMB, BATCH), 1.0, 6.0, ((0, 2), (1, 8), (2, 16))),
        "cross_weight": normal_values(key_of[1], (CROSS, FIELDS, EMB, FIELDS, EMB), (FIELDS * EMB) ** -0.5, 0.109375, ((1, 2), (2, 8))),
        "cross_bias": normal_values(key_of[2], (CROSS, FIELDS, EMB), 0.5, 3.0, ((1, 2), (2, 8)), jnp.float32),
        "tower_weight": normal_values(key_of[3], (TOWER, FIELDS, EMB), (FIELDS * EMB) ** -0.5, 0.109375, ((0, 16),)),
        "tower_bias": normal_values(key_of[4], (TOWER,), 0.5, 3.0, ((0, 16),), jnp.float32),
        "query_weight": normal_values(key_of[5], (TOWER, EMB), TOWER ** -0.5, 0.1875, ((0, 16),)),
        "user_vec": draw_user_vec(jax.random.fold_in(key_of[9], 71), 0),
        "candidates": draw_candidates(jax.random.fold_in(key_of[9], 71), 0),
        "positive": plant(jax.random.randint(key_of[8], (BATCH,), 0, CANDS), jax.random.fold_in(key_of[8], 1), 0, CANDS - 1).astype(jnp.int32),
    }


def reference(features, cross_weight, cross_bias, tower_weight, tower_bias, query_weight, user_vec, candidates, positive):
    width_all = FIELDS * EMB
    anchor = features.reshape(width_all, BATCH).T
    current = anchor
    for level_idx in range(CROSS):
        matrix = cross_weight[level_idx].reshape(width_all, width_all).T
        product = jnp.dot(current, matrix, preferred_element_type=jnp.float32) + cross_bias[level_idx].reshape(width_all)
        current = (anchor.astype(jnp.float32) * product + current.astype(jnp.float32)).astype(jnp.bfloat16)
    crossed = current.T.reshape(FIELDS, EMB, BATCH)
    tower_matrix = tower_weight.reshape(TOWER, width_all).T
    hidden = jax.nn.relu(jnp.dot(current, tower_matrix, preferred_element_type=jnp.float32) + tower_bias).astype(jnp.bfloat16)
    query_vec = (jnp.dot(hidden, query_weight, preferred_element_type=jnp.float32) + user_vec.astype(jnp.float32)).astype(jnp.bfloat16)
    score_scale = 1.0 / math.sqrt(EMB)

    def block_loss(inputs):
        queries, targets = inputs
        logits = jnp.dot(queries, candidates.T, preferred_element_type=jnp.float32) * score_scale
        picked = jnp.take_along_axis(logits, targets[:, None], axis=1)[:, 0]
        return jax.nn.logsumexp(logits, axis=1) - picked
    losses = lax.map(block_loss, (query_vec.reshape(N_BATCH, EX_DEV, EMB), positive.reshape(N_BATCH, EX_DEV)))
    return (crossed, losses.reshape(BATCH))
```

```python
import functools
import math

import jax
import jax.numpy as jnp
from jax import lax
from jax.experimental import pallas as pl
from jax.experimental.pallas import tpu as pltpu
from jax.sharding import Mesh
from jax.sharding import PartitionSpec as P

BATCH = ("batch_0", "batch_1")
MESH = pl.DeviceIdType.MESH
F32 = jnp.float32
BF16 = jnp.bfloat16

FIELDS = 26
NX = 4
NZ = 8
HALF = 13
SUB = 16
BLK = 7
NY = 6
NREST = FIELDS + 1 - NX * NY
KB = FIELDS + 1
KA = NY * 128
KR = NREST * 128
KW = KB * 128
QUART = 52
TC = BLK * 128 + 256
UNITS = 1024


def copy(src, dst, send, recv, where):
    return pltpu.make_async_remote_copy(
        src_ref=src, dst_ref=dst, send_sem=send, recv_sem=recv, device_id=where, device_id_type=MESH
    )


def arrived(ref, sem):
    pltpu.make_async_copy(ref, ref, sem).wait()


def slot_shift(s):
    return jnp.where(s % 2 == 1, (s + 1) // 2, (NZ - s // 2) % NZ)


def kernel(
    feat, w_own, t_own, c_own, user_t, target,
    out, loss,
    a1, a2, w, t, cur1, cur2, part, mine, rs, cands, logits,
    a2a_s, a2a_r, ag1_s, ag1_r, ag1_ls, ag2_s, ag2_r, ag2_ls, ag2_lr,
    z_s, z_r, y_s, y_r, l_s, l_r, d_s, d_r,
    t_s, t_r, td_s, td_r, c_s, c_r, rs_s, rs_r, o_s, o_r, g_s, g_r,
):
    x = lax.axis_index("batch_1")
    y = lax.axis_index("batch_0")
    z = lax.axis_index("dim")
    c = lax.axis_index("field")
    p = x % 2
    wide = x // 2
    tall = 1 - wide
    xr, xl = (x + 1) % NX, (x + NX - 1) % NX
    yr, yl = (y + 1) % NX, (y + NX - 1) % NX
    zr, zl = (z + 1) % NZ, (z + NZ - 1) % NZ
    first = 2 * (1 - c)

    def lanes(j):
        return pl.ds(pl.multiple_of(j * 128, 128), 128)

    def ycols(who):
        return pl.ds(pl.multiple_of(who * KA, 128), KA)

    rest = pl.ds(NX * NY * 128, KR)

    @pl.loop(1, NZ)
    def _(dz):
        to = (z + dz) % NZ
        copy(
            feat.at[:, :, lanes(to)],
            a1.at[pl.ds(HALF * c, HALF), z, :, lanes(p)],
            a2a_s.at[0], a2a_r.at[dz], {"dim": to, "field": tall},
        ).start()

    @pl.when(c == wide)
    def _():
        copy(
            feat.at[:, :, lanes(z)],
            a1.at[pl.ds(HALF * c, HALF), z, :, lanes(p)],
            a2a_s.at[1], a2a_r.at[0], {"field": tall},
        ).start()

    @pl.when(c == tall)
    def _():
        a1[pl.ds(HALF * c, HALF), z, :, lanes(p)] = feat[:, :, lanes(z)]
        cands[NX * y + x] = c_own[...]
        for step in range(1, NX):
            to = (x + step) % NX
            copy(
                c_own, cands.at[NX * y + x], c_s.at[0], c_r.at[0], {"batch_1": to, "field": 1 - to // 2}
            ).start()

    row = lax.broadcasted_iota(jnp.int32, (NZ, SUB, 256), 0) * SUB + lax.broadcasted_iota(
        jnp.int32, (NZ, SUB, 256), 1
    )
    ones = jnp.where(row < 3, 1.0, 0.0).astype(BF16)
    a1[FIELDS] = ones
    a2[FIELDS * NZ : KB * NZ] = ones
    t[z, c] = t_own[...]

    def from_z(level, s):
        src = (z + NZ - slot_shift(s)) % NZ
        own = w.at[level, :, src, :, ycols(y)]
        tail = w.at[level, :, src, :, rest]

        def on(ref, k, d):
            to = jnp.where(d == 0, zr, zl)
            nxt = jnp.where(s == 0, 1 + d, jnp.minimum(s + 2, NZ - 1))
            copy(ref, ref, z_s.at[level, d, k], z_r.at[level, nxt, k], {"dim": to}).start()

        d = jnp.where(s % 2 == 1, 0, 1)

        @pl.when(s > 0)
        def _():
            arrived(own, z_r.at[level, s, 0])

        @pl.when((s > 0) & (s < 6))
        def _():
            on(own, 0, d)

        @pl.when(s == 0)
        def _():
            on(own, 0, 0)
            on(own, 0, 1)

        copy(own, own, y_s.at[level, 0], y_r.at[level, s, 0], {"batch_0": yr}).start()
        copy(own, own, y_s.at[level, 1], y_r.at[level, s, 1], {"batch_0": yl}).start()

        @pl.when(s > 0)
        def _():
            arrived(tail, z_r.at[level, s, 1])

        @pl.when((s > 0) & ((s < 5) | (s == 6)))
        def _():
            on(tail, 1, d)

        @pl.when(s == 0)
        def _():
            on(tail, 1, 0)
            on(tail, 1, 1)

    def from_y(level, s):
        src = (z + NZ - slot_shift(s)) % NZ
        left = w.at[level, :, src, :, ycols(yl)]
        right = w.at[level, :, src, :, ycols(yr)]
        arrived(left, y_r.at[level, s, 0])
        up = w.at[level, pl.ds(0, 4), src, :, ycols(yl)]
        copy(up, up, l_s.at[level, 0], l_r.at[level, s, 0], {"batch_0": yr}).start()
        arrived(right, y_r.at[level, s, 1])
        down = w.at[level, pl.ds(4, 3), src, :, ycols(yr)]
        copy(down, down, l_s.at[level, 1], l_r.at[level, s, 1], {"batch_0": yl}).start()

    def to_core(level, s):
        src = (z + NZ - slot_shift(s)) % NZ
        far = (y + 2) % NX
        arrived(w.at[level, pl.ds(0, 4), src, :, ycols(far)], l_r.at[level, s, 0])
        arrived(w.at[level, pl.ds(4, 3), src, :, ycols(far)], l_r.at[level, s, 1])
        piece = w.at[level, :, src]
        copy(piece, piece, d_s.at[level], d_r.at[level], {"field": 1 - c}).start()

    def tower_step(s):
        src = (z + NZ - slot_shift(s)) % NZ
        whole = t.at[src, c]

        @pl.when(s == 0)
        def _():
            copy(whole, whole, t_s.at[0], t_r.at[1], {"dim": zr}).start()
            copy(whole, whole, t_s.at[1], t_r.at[2], {"dim": zl}).start()

        @pl.when((s > 0) & (s < 7))
        def _():
            arrived(whole, t_r.at[s])

        for par, to in ((1, zr), (0, zl)):
            d = 1 - par
            half = t.at[src, c, pl.ds(32 * d, 32)]

            @pl.when((s > 0) & (s < 5) & (s % 2 == par))
            def _():
                copy(whole, whole, t_s.at[d], t_r.at[s + 2], {"dim": to}).start()

            @pl.when(s == 6 - par)
            def _():
                copy(half, half, t_s.at[2 + d], t_r.at[7 + d], {"dim": to}).start()

        @pl.when(s == 7)
        def _():
            arrived(t.at[src, c, pl.ds(0, 32)], t_r.at[7])
            arrived(t.at[src, c, pl.ds(32, 32)], t_r.at[8])

        copy(whole, whole, td_s, td_r, {"field": 1 - c}).start()

    def example_step(s):
        dz = slot_shift(s)
        src = (z + NZ - dz) % NZ
        whole = a1.at[pl.ds(0, FIELDS), src, :, lanes(p)]

        @pl.when(s == 0)
        def _():
            arrived(a1.at[pl.ds(0, HALF), src, :, lanes(p)], a2a_r.at[0])

        @pl.when(s > 0)
        def _():
            arrived(whole, a2a_r.at[dz])

        copy(whole, whole, ag1_s.at[0], ag1_r.at[p, s, 0], {"batch_1": xr}).start()
        copy(whole, whole, ag1_s.at[1], ag1_r.at[p, s, 1], {"batch_1": xl}).start()

    def relay_step(s):
        src = (z + NZ - slot_shift(s)) % NZ
        for j in range(2):
            r = (x + NX - first - j) % NX
            whole = a1.at[pl.ds(0, FIELDS), src, :, pl.ds(128 * j, 128)]

            @pl.when(r == 1)
            def _():
                arrived(whole, ag1_r.at[j, s, 0])
                half = a1.at[pl.ds(0, HALF), src, :, pl.ds(128 * j, 128)]
                copy(half, half, ag1_ls.at[0], ag1_r.at[j, s, 0], {"batch_1": xr}).start()

            @pl.when(r == 3)
            def _():
                arrived(whole, ag1_r.at[j, s, 1])
                half = a1.at[pl.ds(HALF, HALF), src, :, pl.ds(128 * j, 128)]
                copy(half, half, ag1_ls.at[1], ag1_r.at[j, s, 1], {"batch_1": xl}).start()

    def far_step(s):
        src = (z + NZ - slot_shift(s)) % NZ
        for j in range(2):
            r = (x + NX - first - j) % NX

            @pl.when(r == 2)
            def _():
                arrived(a1.at[pl.ds(0, HALF), src, :, pl.ds(128 * j, 128)], ag1_r.at[j, s, 0])
                arrived(a1.at[pl.ds(HALF, HALF), src, :, pl.ds(128 * j, 128)], ag1_r.at[j, s, 1])

    def tiles(who, h):
        return a2.at[pl.ds(QUART * who + 26 * h, 26)]

    def second_send():
        for h in range(2):
            mineh = cur1.at[pl.ds(4 * p + 26 * h, 26)]
            copy(mineh, tiles(x, h), ag2_s.at[h, 0], ag2_r.at[h, 0], {"batch_1": xr}).start()
            copy(mineh, tiles(x, h), ag2_s.at[h, 1], ag2_r.at[h, 1], {"batch_1": xl}).start()

    def second_step(h):
        for d in ((0, 1) if h == 0 else (1, 0)):
            who, to = ((xl, xr), (xr, xl))[d]
            arrived(tiles(who, h), ag2_r.at[h, d])
            if d == h:
                copy(tiles(who, h), tiles(who, h), ag2_ls.at[h], ag2_lr.at[h], {"batch_1": to}).start()

    def second_far():
        far = (x + 2) % NX
        arrived(tiles(far, 0), ag2_lr.at[0])
        arrived(tiles(far, 1), ag2_lr.at[1])

    @pl.when(c == wide)
    def _():
        w[:, :, z, :, ycols(y)] = w_own[:, :, :, 0:KA]
        w[:, :, z, :, NX * NY * 128 :] = w_own[:, :, :, KA:]

        @pl.loop(0, NZ + 2)
        def _(i):
            @pl.when(i < NZ)
            def _():
                from_z(0, i)

            @pl.when((i > 0) & (i < NZ + 1))
            def _():
                from_y(0, i - 1)

            @pl.when(i > 1)
            def _():
                to_core(0, i - 2)

            @pl.when(i < NZ)
            def _():
                relay_step(i)

        from_z(1, 0)

        @pl.loop(0, NZ)
        def _(i):
            far_step(i)

    @pl.when(c == tall)
    def _():
        @pl.loop(0, NZ)
        def _(i):
            example_step(i)
            relay_step(i)

        tower_step(0)
        arrived(w.at[0], d_r.at[0])

    base = HALF * wide + 6 * p

    @pl.loop(0, BLK)
    def _(f):
        lhs = w[0, f].reshape(128, KW)
        prod = jnp.dot(lhs, a1[...].reshape(KW, 256), preferred_element_type=F32)
        anchor = a1[base + f].reshape(128, 256).astype(F32)
        nxt = (anchor * prod + anchor).astype(BF16)
        cur1[pl.ds(NZ * f, NZ)] = nxt.reshape(NZ, SUB, 256)

    second_send()
    a2[pl.ds(QUART * x, QUART)] = cur1[pl.ds(4 * p, QUART)]

    @pl.when(c == wide)
    def _():
        tower_step(0)

        @pl.loop(1, NZ + 2)
        def _(i):
            @pl.when(i < NZ)
            def _():
                from_z(1, i)

            from_y_ok = i < NZ + 1

            @pl.when(from_y_ok)
            def _():
                from_y(1, i - 1)

            @pl.when(i > 1)
            def _():
                to_core(1, i - 2)

            @pl.when(i < NZ)
            def _():
                tower_step(i)

            @pl.when(i == 3)
            def _():
                second_step(0)

            @pl.when(i == 6)
            def _():
                second_step(1)

        second_far()

    @pl.when(c == tall)
    def _():
        got = cands.at[pl.ds(NX * y, NX)]
        arrived(cands.at[pl.ds(NX * y, NX - 1)], c_r.at[0])
        for step in range(1, NX):
            copy(got, got, c_s.at[1], c_r.at[1], {"batch_0": (y + step) % NX}).start()

        @pl.loop(1, NZ)
        def _(i):
            tower_step(i)

            @pl.when(i == 3)
            def _():
                second_step(0)

            @pl.when(i == 5)
            def _():
                second_step(1)

        second_far()
        arrived(w.at[1], d_r.at[1])

    @pl.loop(0, BLK)
    def _(f):
        lhs = w[1, f].reshape(128, KW)
        prod = jnp.dot(lhs, a2[...].reshape(KW, 256), preferred_element_type=F32)
        anchor = a1[base + f].reshape(128, 256).astype(F32)
        before = cur1[pl.ds(NZ * f, NZ)].reshape(128, 256).astype(F32)
        nxt = (anchor * prod + before).astype(BF16)
        cur2[f] = nxt.reshape(NZ, SUB, 256)

    arrived(t.at[:, c], td_r)

    @pl.loop(0, NZ)
    def _(k):
        lhs = t[k, :, :, 0 : BLK * 128].reshape(128, BLK * 128)
        prod = jnp.dot(lhs, cur2[...].reshape(BLK * 128, 256), preferred_element_type=F32)
        part[pl.ds(128 * k, 128)] = prod.astype(BF16)
        mine[pl.ds(128 * k, 128)] = prod

    for j in range(2):
        @pl.when(x != first + j)
        def _():
            r = (x + NX - first - j) % NX
            copy(
                part.at[:, pl.ds(128 * j, 128)], rs.at[r - 1], rs_s.at[j], rs_r, {"batch_1": first + j}
            ).start()

    @pl.loop(0, 2 * NZ)
    def _(i):
        j, to = i // NZ, i % NZ
        where = {"batch_1": first + j, "dim": to, "field": wide}
        copy(
            cur2.at[pl.ds(p, 6), to, :, lanes(j)],
            out.at[pl.ds(7 * p, 6), :, lanes(z)],
            o_s.at[0], o_r, where,
        ).start()

        @pl.when((to // 4) == p)
        def _():
            copy(
                cur2.at[pl.ds(6 - 6 * p, 1), to, :, lanes(j)],
                out.at[pl.ds(6, 1), :, lanes(z)],
                o_s.at[1], o_r, where,
            ).start()

    @pl.when(c == tall)
    def _():
        arrived(rs, rs_r)
        here = lanes(p)
        bias = t[:, :, :, BLK * 128 + 128 :].reshape(UNITS, 128).astype(F32)
        bias = bias[:, 0:1] + bias[:, 1:2] + bias[:, 2:3]
        total = mine[:, here] + rs[0].astype(F32) + rs[1].astype(F32) + rs[2].astype(F32)
        hidden = jnp.maximum(total + bias, 0.0).astype(BF16)
        qw = t[:, :, :, BLK * 128 : BLK * 128 + 128].reshape(UNITS, 128)
        query = lax.dot_general(qw, hidden, (((0,), (0,)), ((), ())), preferred_element_type=F32)
        query = (query + user_t[...].astype(F32)).astype(BF16)

        arrived(cands.at[pl.ds(0, 3 * NX)], c_r.at[1])
        scale = 1.0 / math.sqrt(128)

        def scores(k, top):
            got = jnp.dot(cands[k], query, preferred_element_type=F32) * scale
            logits[k] = got
            return jnp.maximum(top, jnp.max(got.reshape(32, 8, 128), axis=0))

        top = lax.fori_loop(0, NX * NX, scores, jnp.full((8, 128), -1e30, F32))
        top = jnp.max(top, axis=0, keepdims=True)
        wanted = target[0:1, :]
        index = lax.broadcasted_iota(jnp.int32, (256, 128), 0)

        def sums(k, carry):
            total, picked = carry
            got = logits[k]
            e = jnp.exp(got - top)
            hit = jnp.where(index == wanted - 256 * k, got, 0.0)
            return (
                total + jnp.sum(e.reshape(32, 8, 128), axis=0),
                picked + jnp.sum(hit.reshape(32, 8, 128), axis=0),
            )

        zero = jnp.zeros((8, 128), F32)
        total, picked = lax.fori_loop(0, NX * NX, sums, (zero, zero))
        total = jnp.sum(total, axis=0, keepdims=True)
        picked = jnp.sum(picked, axis=0, keepdims=True)
        result = top + jnp.log(total) - picked
        loss[z] = jnp.broadcast_to(result, (8, 128))

        @pl.loop(1, NZ)
        def _(dz):
            to = (z + dz) % NZ
            copy(loss.at[z], loss.at[z], g_s.at[0], g_r, {"dim": to}).start()
            copy(loss.at[z], loss.at[z], g_s.at[1], g_r, {"dim": to, "field": wide}).start()

        copy(loss.at[z], loss.at[z], g_s.at[2], g_r, {"field": wide}).start()
        arrived(loss.at[pl.ds(0, NZ - 1)], g_r)
        arrived(loss.at[pl.ds(0, NZ - 1)], g_s.at[0])
        arrived(loss.at[pl.ds(0, NZ - 1)], g_s.at[1])
        arrived(loss.at[0], g_s.at[2])
        arrived(cands.at[pl.ds(0, 3)], c_s.at[0])
        arrived(cands.at[pl.ds(0, 3 * NX)], c_s.at[1])
        for d in range(2):
            arrived(a1.at[pl.ds(0, FIELDS), :, :, pl.ds(0, 128)], ag1_s.at[d])

    @pl.when(c == wide)
    def _():
        arrived(loss, g_r)
        arrived(feat.at[:, :, pl.ds(0, 128)], a2a_s.at[1])
        for level in range(2):
            arrived(w.at[level, :, pl.ds(0, 4), :, pl.ds(0, KA)], z_s.at[level, 0, 0])
            arrived(w.at[level, :, pl.ds(0, 3), :, pl.ds(0, KA)], z_s.at[level, 1, 0])
            arrived(w.at[level, :, pl.ds(0, 3), :, rest], z_s.at[level, 0, 1])
            arrived(w.at[level, :, pl.ds(0, 4), :, rest], z_s.at[level, 1, 1])
            arrived(w.at[level, :, :, :, pl.ds(0, KA)], y_s.at[level, 0])
            arrived(w.at[level, :, :, :, pl.ds(0, KA)], y_s.at[level, 1])
            arrived(w.at[level, pl.ds(0, 4), :, :, pl.ds(0, KA)], l_s.at[level, 0])
            arrived(w.at[level, pl.ds(4, 3), :, :, pl.ds(0, KA)], l_s.at[level, 1])
            arrived(w.at[level], d_s.at[level])

    arrived(feat.at[:, :, pl.ds(0, 128 * (NZ - 1))], a2a_s.at[0])
    for j in range(2):
        r = (x + NX - first - j) % NX

        @pl.when(r == 1)
        def _():
            arrived(a1.at[pl.ds(0, HALF), :, :, pl.ds(0, 128)], ag1_ls.at[0])

        @pl.when(r == 3)
        def _():
            arrived(a1.at[pl.ds(0, HALF), :, :, pl.ds(0, 128)], ag1_ls.at[1])

        @pl.when(r != 0)
        def _():
            arrived(rs.at[0], rs_s.at[j])

    for h in range(2):
        for d in range(2):
            arrived(tiles(0, h), ag2_s.at[h, d])
        arrived(tiles(0, h), ag2_ls.at[h])
    for d in range(2):
        arrived(t.at[pl.ds(0, 3), 0], t_s.at[d])
        arrived(t.at[0, 0, pl.ds(0, 32)], t_s.at[2 + d])
    arrived(t.at[:, 0], td_s)
    arrived(cur2.at[pl.ds(0, 6)], o_s.at[0])
    arrived(cur2.at[0, pl.ds(0, 4)], o_s.at[1])
    arrived(out, o_r)


def three_parts(v):
    hi = lax.reduce_precision(v, 8, 7)
    mid = lax.reduce_precision(v - hi, 8, 7)
    low = (v - hi) - mid
    return jnp.stack([hi, mid, low], axis=-1).astype(BF16)


def lane_block(parts):
    return jnp.pad(parts, [(0, 0)] * (parts.ndim - 1) + [(0, 128 - parts.shape[-1])])


def body(features, cross_weight, cross_bias, tower_weight, tower_bias, query_weight, user_vec, candidates, positive):
    x = lax.axis_index("batch_1")
    y = lax.axis_index("batch_0")
    z = lax.axis_index("dim")
    p = x % 2

    rows = lax.dynamic_slice_in_dim(cross_weight, 6 * p, BLK, 1)
    own = lax.dynamic_slice_in_dim(rows, NY * y, NY, 3)
    rest = rows[:, :, :, NX * NY :]
    bias = lane_block(three_parts(lax.dynamic_slice_in_dim(cross_bias, 6 * p, BLK, 1)))
    w_own = jnp.concatenate([own, rest, bias[:, :, :, None]], axis=3).reshape(2, BLK, SUB, KA + KR)

    cols = lax.dynamic_slice_in_dim(tower_weight, (13 * x) // 2, BLK, 1).reshape(64, BLK * 128)
    at = lax.broadcasted_iota(jnp.int32, (1, BLK * 128), 1) - 64 * p
    cols = jnp.where((at >= 0) & (at < 832), cols, jnp.zeros_like(cols))
    t_own = jnp.concatenate([cols, query_weight, lane_block(three_parts(tower_bias))], axis=1)

    user_t = lax.dynamic_slice_in_dim(user_vec, 128 * z, 128, 0).T
    target = jnp.broadcast_to(lax.dynamic_slice_in_dim(positive, 128 * z, 128, 0)[None], (8, 128))

    vmem = pl.BlockSpec(memory_space=pltpu.VMEM)
    dma = pltpu.SemaphoreType.DMA
    out, loss = pl.pallas_call(
        kernel,
        out_shape=(
            jax.ShapeDtypeStruct((HALF, SUB, 1024), BF16),
            jax.ShapeDtypeStruct((NZ, 8, 128), F32),
        ),
        in_specs=[vmem] * 6,
        out_specs=(vmem, vmem),
        scratch_shapes=[
            pltpu.VMEM((KB, NZ, SUB, 256), BF16),
            pltpu.VMEM((KB * NZ, SUB, 256), BF16),
            pltpu.VMEM((2, BLK, NZ, SUB, KW), BF16),
            pltpu.VMEM((NZ, 2, 64, TC), BF16),
            pltpu.VMEM((BLK * NZ, SUB, 256), BF16),
            pltpu.VMEM((BLK, NZ, SUB, 256), BF16),
            pltpu.VMEM((UNITS, 256), BF16),
            pltpu.VMEM((UNITS, 256), F32),
            pltpu.VMEM((3, UNITS, 128), BF16),
            pltpu.VMEM((NX * NX, 256, 128), BF16),
            pltpu.VMEM((NX * NX, 256, 128), F32),
            dma((2,)), dma((NZ,)),
            dma((2,)), dma((2, NZ, 2)), dma((2,)),
            dma((2, 2)), dma((2, 2)), dma((2,)), dma((2,)),
            dma((2, 2, 2)), dma((2, NZ, 2)),
            dma((2, 2)), dma((2, NZ, 2)),
            dma((2, 2)), dma((2, NZ, 2)),
            dma((2,)), dma((2,)),
            dma((4,)), dma((9,)), dma, dma,
            dma((2,)), dma((2,)),
            dma((2,)), dma,
            dma((2,)), dma,
            dma((3,)), dma,
        ],
        compiler_params=pltpu.CompilerParams(has_side_effects=True, vmem_limit_bytes=60 * 1024 * 1024),
        name="dcn",
    )(features, w_own, t_own, candidates, user_t, target)
    return out, loss[:, 0, :].reshape(1024)


def solution(mesh):
    torus = Mesh(
        mesh.devices.reshape(4, 4, mesh.shape["field"], mesh.shape["dim"]),
        ("batch_0", "batch_1", "field", "dim"),
    )
    in_specs = (
        P("field", "dim", BATCH),
        P(None, "field", "dim", None, None),
        P(None, "field", "dim"),
        P(("field", "dim"), None, None),
        P(("field", "dim")),
        P(("field", "dim"), None),
        P(BATCH, None),
        P(BATCH, None),
        P(BATCH),
    )
    out_specs = (P("field", "dim", BATCH), P(BATCH))
    return jax.shard_map(body, mesh=torus, in_specs=in_specs, out_specs=out_specs, check_vma=False)
```

```python
import functools
import math

import jax
import jax.numpy as jnp
from jax import lax
from jax.experimental import pallas as pl
from jax.experimental.pallas import tpu as pltpu
from jax.sharding import Mesh
from jax.sharding import PartitionSpec as P

BATCH = ("batch_0", "batch_1")
MESH = pl.DeviceIdType.MESH
F32 = jnp.float32
BF16 = jnp.bfloat16

FIELDS = 26
NX = 4
NZ = 8
HALF = 13
SUB = 16
BLK = 7
NY = 6
NREST = FIELDS + 1 - NX * NY
KB = FIELDS + 1
KA = NY * 128
KR = NREST * 128
KW = KB * 128
QUART = 52
TC = BLK * 128 + 256
UNITS = 1024


def copy(src, dst, send, recv, where):
    return pltpu.make_async_remote_copy(
        src_ref=src, dst_ref=dst, send_sem=send, recv_sem=recv, device_id=where, device_id_type=MESH
    )


def arrived(ref, sem):
    pltpu.make_async_copy(ref, ref, sem).wait()


def slot_shift(s):
    return jnp.where(s % 2 == 1, (s + 1) // 2, (NZ - s // 2) % NZ)


def kernel(
    feat, c_w, c_b, t_w, t_b, q_w, c_own, user, target,
    out, loss_out,
    a1, a2, w, t, cur1, cur2, part, mine, rs, hop, summed, cands, logits, u_own, loss,
    w_l, t_l, u_l,
    a2a_s, a2a_r, ag1_s, ag1_r, ag1_ls, ag2_s, ag2_r, ag2_ls, ag2_lr,
    z_s, z_r, y_s, y_r, l_s, l_r, da_s, da_r, db_s, db_r, dy_s, dy_r,
    t_s, t_r, td_s, td_r, c_s, c_r, rs_s, rs_r, hop_r, o_s, o_r, g_s, g_r,
):
    x = lax.axis_index("batch_1")
    y = lax.axis_index("batch_0")
    z = lax.axis_index("dim")
    c = lax.axis_index("field")
    p = x % 2
    wide = x // 2
    tall = 1 - wide
    xr, xl = (x + 1) % NX, (x + NX - 1) % NX
    yr, yl = (y + 1) % NX, (y + NX - 1) % NX
    zr, zl = (z + 1) % NZ, (z + NZ - 1) % NZ
    first = 2 * (1 - c)

    def lanes(j):
        return pl.ds(pl.multiple_of(j * 128, 128), 128)

    def ycols(who):
        return pl.ds(pl.multiple_of(who * KA, 128), KA)

    rest = pl.ds(NX * NY * 128, KR)

    barrier = pltpu.get_barrier_semaphore()

    def greet(where):
        pl.semaphore_signal(barrier, inc=1, device_id=where, device_id_type=MESH)

    for step in range(1, NX):
        for core in range(2):
            greet({"batch_1": (x + step) % NX, "field": core})
        greet({"batch_0": (y + step) % NX})
    for step in range(1, NZ):
        for core in range(2):
            greet({"dim": (z + step) % NZ, "field": core})
    greet({"field": 1 - c})

    base = HALF * wide + 6 * p
    own_w = [(level, k) for level in range(2) for k in range(NY + NREST - 1)]

    def own_copy(level, k):
        field = NY * y + k if k < NY else NX * NY + k - NY
        return pltpu.make_async_copy(
            c_w.at[level, pl.ds(6 * p, BLK), field], w.at[level, :, z, :, lanes(field)], w_l.at[level, k]
        )

    @pl.when(c == wide)
    def _():
        for level, k in own_w:
            own_copy(level, k).start()

    t_copies = [
        pltpu.make_async_copy(t_w.at[base + k], t.at[z, c, :, pl.ds(128 * k, 128)], t_l.at[k])
        for k in range(BLK)
    ]
    for cp in t_copies:
        cp.start()

    u_copy = pltpu.make_async_copy(user.at[pl.ds(pl.multiple_of(128 * z, 128), 128)], u_own, u_l)

    @pl.when(c == tall)
    def _():
        u_copy.start()

    row = lax.broadcasted_iota(jnp.int32, (NZ, SUB, 256), 0) * SUB + lax.broadcasted_iota(
        jnp.int32, (NZ, SUB, 256), 1
    )
    ones = jnp.where(row < 3, 1.0, 0.0).astype(BF16)
    a1[FIELDS] = ones
    a2[FIELDS * NZ : KB * NZ] = ones

    def bias_block(values):
        n = values.shape[1]
        eye = lax.broadcasted_iota(jnp.int32, (n, n), 0) == lax.broadcasted_iota(jnp.int32, (n, n), 1)
        col = jnp.sum(jnp.where(eye, values, 0.0), axis=1, keepdims=True)
        hi = col.astype(BF16).astype(F32)
        mid = (col - hi).astype(BF16).astype(F32)
        low = (col - hi) - mid
        lane = lax.broadcasted_iota(jnp.int32, (n, 128), 1)
        terms = jnp.where(lane == 0, hi, jnp.where(lane == 1, mid, jnp.where(lane == 2, low, 0.0)))
        return terms.astype(BF16)

    t[z, c, :, BLK * 128 : BLK * 128 + 128] = q_w[...]
    t[z, c, :, BLK * 128 + 128 :] = bias_block(t_b[...])

    @pl.when(c == wide)
    def _():
        @pl.loop(0, BLK)
        def _(f):
            for level in range(2):
                w[level, f, z, :, FIELDS * 128 :] = bias_block(c_b[6 * p + f, level : level + 1])

        for level, k in own_w:
            own_copy(level, k).wait()

    @pl.when(c == tall)
    def _():
        a1[pl.ds(HALF * c, HALF), z, :, lanes(p)] = feat[:, :, lanes(z)]
        cands[NX * y + x] = c_own[...]

    for cp in t_copies:
        cp.wait()
    lane64 = lax.broadcasted_iota(jnp.int32, (64, 128), 1)
    edge = lanes((BLK - 1) * (1 - p))
    kept = (lane64 < 64) == (p == 0)
    t[z, c, :, edge] = jnp.where(kept, t[z, c, :, edge].astype(F32), 0.0).astype(BF16)

    pl.semaphore_wait(barrier, 3 * NX - 3 + 2 * NZ - 2 + 1)

    def examples_out():
        @pl.loop(1, NZ)
        def _(s):
            to = (z + slot_shift(s)) % NZ
            copy(
                feat.at[:, :, lanes(to)],
                a1.at[pl.ds(HALF * c, HALF), z, :, lanes(p)],
                a2a_s.at[0], a2a_r.at[slot_shift(s)], {"dim": to, "field": tall},
            ).start()

    def along_z(ref, level, s, k, d):
        to = jnp.where(d == 0, zr, zl)
        nxt = jnp.where(s == 0, 1 + d, jnp.minimum(s + 2, NZ - 1))
        copy(ref, ref, z_s.at[level, d, k], z_r.at[level, nxt, k], {"dim": to}).start()

    def from_z(level, s, k):
        src = (z + NZ - slot_shift(s)) % NZ
        ref = w.at[level, :, src, :, rest] if k else w.at[level, :, src, :, ycols(y)]
        onward = ((s < 5) | (s == 6)) if k else (s < 6)

        @pl.when(s > 0)
        def _():
            arrived(ref, z_r.at[level, s, k])

        @pl.when((s > 0) & onward)
        def _():
            along_z(ref, level, s, k, jnp.where(s % 2 == 1, 0, 1))

        @pl.when(s == 0)
        def _():
            along_z(ref, level, s, k, 0)
            along_z(ref, level, s, k, 1)

        if k:
            copy(ref, ref, db_s.at[level], db_r.at[level], {"field": 1 - c}).start()
        else:
            copy(ref, ref, da_s.at[level], da_r.at[level, s], {"field": 1 - c}).start()

    def from_a(level, s):
        from_z(level, s, 0)

    def from_b(level, s):
        from_z(level, s, 1)

    def to_y(level, s):
        src = (z + NZ - slot_shift(s)) % NZ
        own = w.at[level, :, src, :, ycols(y)]
        arrived(own, da_r.at[level, s])
        copy(own, own, y_s.at[level, 0], y_r.at[level, s, 0], {"batch_0": yr}).start()
        copy(own, own, y_s.at[level, 1], y_r.at[level, s, 1], {"batch_0": yl}).start()

    def from_y(level, s):
        src = (z + NZ - slot_shift(s)) % NZ
        left = w.at[level, :, src, :, ycols(yl)]
        right = w.at[level, :, src, :, ycols(yr)]
        up = w.at[level, pl.ds(0, 4), src, :, ycols(yl)]
        down = w.at[level, pl.ds(4, 3), src, :, ycols(yr)]
        arrived(left, y_r.at[level, s, 0])
        copy(up, up, l_s.at[level, 0], l_r.at[level, s, 0], {"batch_0": yr}).start()
        copy(left, left, dy_s.at[level], dy_r.at[level], {"field": 1 - c}).start()
        arrived(right, y_r.at[level, s, 1])
        copy(down, down, l_s.at[level, 1], l_r.at[level, s, 1], {"batch_0": yl}).start()
        copy(right, right, dy_s.at[level], dy_r.at[level], {"field": 1 - c}).start()

    def to_core(level, s):
        src = (z + NZ - slot_shift(s)) % NZ
        far = (y + 2) % NX
        piece = w.at[level, :, src, :, ycols(far)]
        arrived(w.at[level, pl.ds(0, 4), src, :, ycols(far)], l_r.at[level, s, 0])
        arrived(w.at[level, pl.ds(4, 3), src, :, ycols(far)], l_r.at[level, s, 1])
        copy(piece, piece, dy_s.at[level], dy_r.at[level], {"field": 1 - c}).start()

    def tower_step(s):
        src = (z + NZ - slot_shift(s)) % NZ
        whole = t.at[src, c]

        @pl.when(s == 0)
        def _():
            copy(whole, whole, t_s.at[0], t_r.at[1], {"dim": zr}).start()
            copy(whole, whole, t_s.at[1], t_r.at[2], {"dim": zl}).start()

        @pl.when((s > 0) & (s < 7))
        def _():
            arrived(whole, t_r.at[s])

        for par, to in ((1, zr), (0, zl)):
            d = 1 - par
            half = t.at[src, c, pl.ds(32 * d, 32)]

            @pl.when((s > 0) & (s < 5) & (s % 2 == par))
            def _():
                copy(whole, whole, t_s.at[d], t_r.at[s + 2], {"dim": to}).start()

            @pl.when(s == 6 - par)
            def _():
                copy(half, half, t_s.at[2 + d], t_r.at[7 + d], {"dim": to}).start()

        @pl.when(s == 7)
        def _():
            arrived(t.at[src, c, pl.ds(0, 32)], t_r.at[7])
            arrived(t.at[src, c, pl.ds(32, 32)], t_r.at[8])

        copy(whole, whole, td_s, td_r, {"field": 1 - c}).start()

    def example_step(s):
        dz = slot_shift(s)
        src = (z + NZ - dz) % NZ
        whole = a1.at[pl.ds(0, FIELDS), src, :, lanes(p)]

        @pl.when(s == 0)
        def _():
            arrived(a1.at[pl.ds(0, HALF), src, :, lanes(p)], a2a_r.at[0])

        @pl.when(s > 0)
        def _():
            arrived(whole, a2a_r.at[dz])

        copy(whole, whole, ag1_s.at[0], ag1_r.at[p, s, 0], {"batch_1": xr}).start()
        copy(whole, whole, ag1_s.at[1], ag1_r.at[p, s, 1], {"batch_1": xl}).start()

    def relay_step(s):
        src = (z + NZ - slot_shift(s)) % NZ
        for j in range(2):
            r = (x + NX - first - j) % NX
            whole = a1.at[pl.ds(0, FIELDS), src, :, pl.ds(128 * j, 128)]

            @pl.when(r == 1)
            def _():
                arrived(whole, ag1_r.at[j, s, 0])
                half = a1.at[pl.ds(0, HALF), src, :, pl.ds(128 * j, 128)]
                copy(half, half, ag1_ls.at[0], ag1_r.at[j, s, 0], {"batch_1": xr}).start()

            @pl.when(r == 3)
            def _():
                arrived(whole, ag1_r.at[j, s, 1])
                half = a1.at[pl.ds(HALF, HALF), src, :, pl.ds(128 * j, 128)]
                copy(half, half, ag1_ls.at[1], ag1_r.at[j, s, 1], {"batch_1": xl}).start()

    def far_step(s):
        src = (z + NZ - slot_shift(s)) % NZ
        for j in range(2):
            r = (x + NX - first - j) % NX

            @pl.when(r == 2)
            def _():
                arrived(a1.at[pl.ds(0, HALF), src, :, pl.ds(128 * j, 128)], ag1_r.at[j, s, 0])
                arrived(a1.at[pl.ds(HALF, HALF), src, :, pl.ds(128 * j, 128)], ag1_r.at[j, s, 1])

    def tiles(who, h):
        return a2.at[pl.ds(QUART * who + 26 * h, 26)]

    def second_send():
        for h in range(2):
            mineh = cur1.at[pl.ds(4 * p + 26 * h, 26)]
            copy(mineh, tiles(x, h), ag2_s.at[h, 0], ag2_r.at[h, 0], {"batch_1": xr}).start()
            copy(mineh, tiles(x, h), ag2_s.at[h, 1], ag2_r.at[h, 1], {"batch_1": xl}).start()

    def second_step(h):
        for d in ((0, 1) if h == 0 else (1, 0)):
            who, to = ((xl, xr), (xr, xl))[d]
            arrived(tiles(who, h), ag2_r.at[h, d])
            if d == h:
                copy(tiles(who, h), tiles(who, h), ag2_ls.at[h], ag2_lr.at[h], {"batch_1": to}).start()

    def second_far():
        far = (x + 2) % NX
        arrived(tiles(far, 0), ag2_lr.at[0])
        arrived(tiles(far, 1), ag2_lr.at[1])

    @pl.when(c == wide)
    def _():
        from_a(0, 0)
        copy(
            feat.at[:, :, lanes(z)],
            a1.at[pl.ds(HALF * c, HALF), z, :, lanes(p)],
            a2a_s.at[1], a2a_r.at[0], {"field": tall},
        ).start()
        examples_out()

        @pl.loop(1, NZ + 3)
        def _(i):
            @pl.when(i < NZ)
            def _():
                from_a(0, i)

            @pl.when(i > 2)
            def _():
                from_b(0, i - 3)

            @pl.when(i == NZ)
            def _():
                from_a(1, 0)

            @pl.when((i > 1) & (i < NZ + 2))
            def _():
                relay_step(i - 2)

        from_a(1, 1)
        from_a(1, 2)
        from_b(1, 0)
        tower_step(0)

        @pl.loop(0, NZ)
        def _(i):
            far_step(i)

        arrived(w.at[0, :, :, :, pl.ds(0, 3 * KA)], dy_r.at[0])

    @pl.when(c == tall)
    def _():
        examples_out()
        for step in range(1, NX):
            to = (x + step) % NX
            copy(
                c_own, cands.at[NX * y + x], c_s.at[0], c_r.at[0], {"batch_1": to, "field": 1 - to // 2}
            ).start()
        to_y(0, 0)
        example_step(0)

        @pl.loop(1, NZ + 3)
        def _(i):
            @pl.when((i > 1) & (i < NZ))
            def _():
                to_y(0, i)

            @pl.when(i < NZ + 1)
            def _():
                from_y(0, i - 1)

            @pl.when(i == 1)
            def _():
                to_y(0, i)

            @pl.when(i < NZ)
            def _():
                example_step(i)

            @pl.when(i == NZ)
            def _():
                to_y(1, 0)

            @pl.when(i == NZ + 1)
            def _():
                to_y(1, 1)

            @pl.when((i > 1) & (i < NZ + 2))
            def _():
                relay_step(i - 2)

            @pl.when(i > 2)
            def _():
                to_core(0, i - 3)

        tower_step(0)
        arrived(w.at[0, :, :, :, rest], db_r.at[0])

    @pl.loop(0, BLK)
    def _(f):
        lhs = w[0, f].reshape(128, KW)
        prod = jnp.dot(lhs, a1[...].reshape(KW, 256), preferred_element_type=F32)
        anchor = a1[base + f].reshape(128, 256).astype(F32)
        nxt = (anchor * prod + anchor).astype(BF16)
        cur1[pl.ds(NZ * f, NZ)] = nxt.reshape(NZ, SUB, 256)

    second_send()
    a2[pl.ds(QUART * x, QUART)] = cur1[pl.ds(4 * p, QUART)]

    @pl.when(c == wide)
    def _():
        @pl.loop(3, NZ + 3)
        def _(i):
            @pl.when(i < NZ)
            def _():
                from_a(1, i)

            @pl.when(i > 3)
            def _():
                from_b(1, i - 3)
                tower_step(i - 3)

            @pl.when(i == 4)
            def _():
                second_step(0)

            @pl.when(i == 6)
            def _():
                second_step(1)

        second_far()
        arrived(w.at[1, :, :, :, pl.ds(0, 3 * KA)], dy_r.at[1])

    @pl.when(c == tall)
    def _():
        got = cands.at[pl.ds(NX * y, NX)]

        @pl.loop(1, NZ + 3)
        def _(i):
            @pl.when((i > 1) & (i < NZ))
            def _():
                to_y(1, i)

            @pl.when(i < NZ + 1)
            def _():
                from_y(1, i - 1)

            @pl.when(i > 2)
            def _():
                to_core(1, i - 3)

            @pl.when(i > 3)
            def _():
                tower_step(i - 3)

            @pl.when(i == 3)
            def _():
                second_step(0)

            @pl.when(i == 5)
            def _():
                second_step(1)

        arrived(cands.at[pl.ds(NX * y, NX - 1)], c_r.at[0])
        for step in range(1, NX):
            copy(got, got, c_s.at[1], c_r.at[1], {"batch_0": (y + step) % NX}).start()
        second_far()
        arrived(w.at[1, :, :, :, rest], db_r.at[1])

    @pl.loop(0, BLK)
    def _(f):
        lhs = w[1, f].reshape(128, KW)
        prod = jnp.dot(lhs, a2[...].reshape(KW, 256), preferred_element_type=F32)
        anchor = a1[base + f].reshape(128, 256).astype(F32)
        before = cur1[pl.ds(NZ * f, NZ)].reshape(128, 256).astype(F32)
        nxt = (anchor * prod + before).astype(BF16)
        cur2[f] = nxt.reshape(NZ, SUB, 256)

    arrived(t.at[:, c], td_r)

    def tower(k):
        lhs = t[k, :, :, 0 : BLK * 128].reshape(128, BLK * 128)
        prod = jnp.dot(lhs, cur2[...].reshape(BLK * 128, 256), preferred_element_type=F32)
        part[pl.ds(128 * k, 128)] = prod.astype(BF16)
        mine[pl.ds(128 * k, 128)] = prod

    def far_sum(h):
        for j in range(2):
            @pl.when((x + NX - first - j) % NX == 2)
            def _():
                to = (xr, xl)[h]
                copy(
                    part.at[pl.ds(512 * h, 512), pl.ds(128 * j, 128)], hop, rs_s.at[h], hop_r, {"batch_1": to}
                ).start()

    for h in range(2):
        @pl.loop(4 * h, 4 * h + 4)
        def _(k):
            tower(k)

        far_sum(h)

    for r, own, added, way in ((1, 0, 512, xl), (3, 512, 0, xr)):
        for j in range(2):
            @pl.when((x + NX - first - j) % NX == r)
            def _():
                cols = pl.ds(128 * j, 128)
                slot = rs.at[r // 2]
                copy(
                    part.at[pl.ds(own, 512), cols], slot.at[pl.ds(own, 512)], rs_s.at[2], rs_r, {"batch_1": way}
                ).start()
                arrived(hop, hop_r)
                summed[...] = (mine[pl.ds(added, 512), cols] + hop[...].astype(F32)).astype(BF16)
                copy(summed, slot.at[pl.ds(added, 512)], rs_s.at[3], rs_r, {"batch_1": way}).start()

    @pl.when(c == tall)
    def _():
        arrived(rs, rs_r)

    for j in range(2):
        r = (x + NX - first - j) % NX

        @pl.when(r == 2)
        def _():
            arrived(hop, rs_s.at[0])
            arrived(hop, rs_s.at[1])

        @pl.when((r == 1) | (r == 3))
        def _():
            arrived(hop, rs_s.at[2])
            arrived(hop, rs_s.at[3])

    @pl.loop(0, 2 * NZ)
    def _(i):
        j, to = i // NZ, (z + slot_shift(i % NZ)) % NZ
        where = {"batch_1": first + j, "dim": to, "field": wide}
        copy(
            cur2.at[pl.ds(p, 6), to, :, lanes(j)],
            out.at[pl.ds(7 * p, 6), :, lanes(z)],
            o_s.at[0], o_r, where,
        ).start()

        @pl.when((to // 4) == p)
        def _():
            copy(
                cur2.at[pl.ds(6 - 6 * p, 1), to, :, lanes(j)],
                out.at[pl.ds(6, 1), :, lanes(z)],
                o_s.at[1], o_r, where,
            ).start()

    @pl.when(c == tall)
    def _():
        here = lanes(p)
        bias = t[:, :, :, BLK * 128 + 128 :].reshape(UNITS, 128).astype(F32)
        bias = bias[:, 0:1] + bias[:, 1:2] + bias[:, 2:3]
        total = mine[:, here] + rs[0].astype(F32) + rs[1].astype(F32)
        hidden = jnp.maximum(total + bias, 0.0).astype(BF16)
        qw = t[:, :, :, BLK * 128 : BLK * 128 + 128].reshape(UNITS, 128)
        query = lax.dot_general(qw, hidden, (((0,), (0,)), ((), ())), preferred_element_type=F32)
        u_copy.wait()
        query = (query + u_own[...].astype(F32).T).astype(BF16)

        arrived(cands.at[pl.ds(0, 3 * NX)], c_r.at[1])
        scale = 1.0 / math.sqrt(128)

        def scores(k, top):
            got = jnp.dot(cands[k], query, preferred_element_type=F32) * scale
            logits[k] = got
            return jnp.maximum(top, jnp.max(got.reshape(32, 8, 128), axis=0))

        top = lax.fori_loop(0, NX * NX, scores, jnp.full((8, 128), -1e30, F32))
        top = jnp.max(top, axis=0, keepdims=True)
        wanted = target[pl.ds(z, 1), :]
        index = lax.broadcasted_iota(jnp.int32, (256, 128), 0)

        def sums(k, carry):
            total, picked = carry
            got = logits[k]
            e = jnp.exp(got - top)
            hit = jnp.where(index == wanted - 256 * k, got, 0.0)
            return (
                total + jnp.sum(e.reshape(32, 8, 128), axis=0),
                picked + jnp.sum(hit.reshape(32, 8, 128), axis=0),
            )

        zero = jnp.zeros((8, 128), F32)
        total, picked = lax.fori_loop(0, NX * NX, sums, (zero, zero))
        total = jnp.sum(total, axis=0, keepdims=True)
        picked = jnp.sum(picked, axis=0, keepdims=True)
        result = top + jnp.log(total) - picked
        loss[z] = jnp.broadcast_to(result, (8, 128))

        @pl.loop(1, NZ)
        def _(dz):
            to = (z + dz) % NZ
            copy(loss.at[z], loss.at[z], g_s.at[0], g_r, {"dim": to}).start()
            copy(loss.at[z], loss.at[z], g_s.at[1], g_r, {"dim": to, "field": wide}).start()

        copy(loss.at[z], loss.at[z], g_s.at[2], g_r, {"field": wide}).start()
        arrived(loss.at[pl.ds(0, NZ - 1)], g_r)
        arrived(loss.at[pl.ds(0, NZ - 1)], g_s.at[0])
        arrived(loss.at[pl.ds(0, NZ - 1)], g_s.at[1])
        arrived(loss.at[0], g_s.at[2])
        arrived(cands.at[pl.ds(0, 3)], c_s.at[0])
        arrived(cands.at[pl.ds(0, 3 * NX)], c_s.at[1])
        for d in range(2):
            arrived(a1.at[pl.ds(0, FIELDS), :, :, pl.ds(0, 128)], ag1_s.at[d])
        for level in range(2):
            for d in range(2):
                arrived(w.at[level, :, :, :, pl.ds(0, KA)], y_s.at[level, d])
            arrived(w.at[level, pl.ds(0, 4), :, :, pl.ds(0, KA)], l_s.at[level, 0])
            arrived(w.at[level, pl.ds(4, 3), :, :, pl.ds(0, KA)], l_s.at[level, 1])
            arrived(w.at[level, :, :, :, pl.ds(0, 3 * KA)], dy_s.at[level])

    @pl.when(c == wide)
    def _():
        arrived(loss, g_r)
        arrived(feat.at[:, :, pl.ds(0, 128)], a2a_s.at[1])
        for level in range(2):
            arrived(w.at[level, :, pl.ds(0, 4), :, pl.ds(0, KA)], z_s.at[level, 0, 0])
            arrived(w.at[level, :, pl.ds(0, 3), :, pl.ds(0, KA)], z_s.at[level, 1, 0])
            arrived(w.at[level, :, pl.ds(0, 3), :, rest], z_s.at[level, 0, 1])
            arrived(w.at[level, :, pl.ds(0, 4), :, rest], z_s.at[level, 1, 1])
            arrived(w.at[level, :, :, :, pl.ds(0, KA)], da_s.at[level])
            arrived(w.at[level, :, :, :, rest], db_s.at[level])

    arrived(feat.at[:, :, pl.ds(0, 128 * (NZ - 1))], a2a_s.at[0])
    for j in range(2):
        r = (x + NX - first - j) % NX

        @pl.when(r == 1)
        def _():
            arrived(a1.at[pl.ds(0, HALF), :, :, pl.ds(0, 128)], ag1_ls.at[0])

        @pl.when(r == 3)
        def _():
            arrived(a1.at[pl.ds(0, HALF), :, :, pl.ds(0, 128)], ag1_ls.at[1])

    for h in range(2):
        for d in range(2):
            arrived(tiles(0, h), ag2_s.at[h, d])
        arrived(tiles(0, h), ag2_ls.at[h])
    for d in range(2):
        arrived(t.at[pl.ds(0, 3), 0], t_s.at[d])
        arrived(t.at[0, 0, pl.ds(0, 32)], t_s.at[2 + d])
    arrived(t.at[:, 0], td_s)
    arrived(cur2.at[pl.ds(0, 6)], o_s.at[0])
    arrived(cur2.at[0, pl.ds(0, 4)], o_s.at[1])
    for k in range(NZ):
        loss_out[k : k + 1] = loss[k, 0:1]
    arrived(out, o_r)


def body(features, cross_weight, cross_bias, tower_weight, tower_bias, query_weight, user_vec, candidates, positive):
    vmem = pl.BlockSpec(memory_space=pltpu.VMEM)
    hbm = pl.BlockSpec(memory_space=pl.ANY)
    dma = pltpu.SemaphoreType.DMA
    out, loss = pl.pallas_call(
        kernel,
        out_shape=(
            jax.ShapeDtypeStruct((HALF, SUB, 1024), BF16),
            jax.ShapeDtypeStruct((NZ, 128), F32),
        ),
        in_specs=[vmem, hbm, vmem, hbm, vmem, vmem, vmem, hbm, vmem],
        out_specs=(vmem, vmem),
        scratch_shapes=[
            pltpu.VMEM((KB, NZ, SUB, 256), BF16),
            pltpu.VMEM((KB * NZ, SUB, 256), BF16),
            pltpu.VMEM((2, BLK, NZ, SUB, KW), BF16),
            pltpu.VMEM((NZ, 2, 64, TC), BF16),
            pltpu.VMEM((BLK * NZ, SUB, 256), BF16),
            pltpu.VMEM((BLK, NZ, SUB, 256), BF16),
            pltpu.VMEM((UNITS, 256), BF16),
            pltpu.VMEM((UNITS, 256), F32),
            pltpu.VMEM((2, UNITS, 128), BF16),
            pltpu.VMEM((UNITS // 2, 128), BF16),
            pltpu.VMEM((UNITS // 2, 128), BF16),
            pltpu.VMEM((NX * NX, 256, 128), BF16),
            pltpu.VMEM((NX * NX, 256, 128), F32),
            pltpu.VMEM((128, 128), BF16),
            pltpu.VMEM((NZ, 8, 128), F32),
            dma((2, NY + NREST - 1)), dma((BLK,)), dma,
            dma((2,)), dma((NZ,)),
            dma((2,)), dma((2, NZ, 2)), dma((2,)),
            dma((2, 2)), dma((2, 2)), dma((2,)), dma((2,)),
            dma((2, 2, 2)), dma((2, NZ, 2)),
            dma((2, 2)), dma((2, NZ, 2)),
            dma((2, 2)), dma((2, NZ, 2)),
            dma((2,)), dma((2, NZ)), dma((2,)), dma((2,)), dma((2,)), dma((2,)),
            dma((4,)), dma((9,)), dma, dma,
            dma((2,)), dma((2,)),
            dma((4,)), dma, dma,
            dma((2,)), dma,
            dma((3,)), dma,
        ],
        compiler_params=pltpu.CompilerParams(collective_id=0, has_side_effects=True, vmem_limit_bytes=60 * 1024 * 1024),
        name="dcn",
    )(
        features,
        cross_weight.transpose(0, 1, 3, 2, 4),
        cross_bias.transpose(1, 0, 2),
        tower_weight.transpose(1, 0, 2),
        tower_bias.reshape(1, 64),
        query_weight,
        candidates,
        user_vec,
        positive.reshape(NZ, 128),
    )
    return out, loss.reshape(1024)


def solution(mesh):
    torus = Mesh(
        mesh.devices.reshape(4, 4, mesh.shape["field"], mesh.shape["dim"]),
        ("batch_0", "batch_1", "field", "dim"),
    )
    in_specs = (
        P("field", "dim", BATCH),
        P(None, "field", "dim", None, None),
        P(None, "field", "dim"),
        P(("field", "dim"), None, None),
        P(("field", "dim")),
        P(("field", "dim"), None),
        P(BATCH, None),
        P(BATCH, None),
        P(BATCH),
    )
    out_specs = (P("field", "dim", BATCH), P(BATCH))
    return jax.shard_map(body, mesh=torus, in_specs=in_specs, out_specs=out_specs, check_vma=False)
```

```python
import functools
import math

import jax
import jax.numpy as jnp
from jax import lax
from jax.experimental import pallas as pl
from jax.experimental.pallas import tpu as pltpu
from jax.sharding import Mesh
from jax.sharding import PartitionSpec as P

BATCH = ("batch_0", "batch_1")
MESH = pl.DeviceIdType.MESH
F32 = jnp.float32
BF16 = jnp.bfloat16

FIELDS = 26
NX = 4
NZ = 8
HALF = 13
SUB = 16
BLK = 7
NY = 6
NREST = FIELDS + 1 - NX * NY
KB = FIELDS + 1
KA = NY * 128
KR = NREST * 128
KW = KB * 128
QUART = 52
TC = BLK * 128 + 256
UNITS = 1024


def copy(src, dst, send, recv, where):
    return pltpu.make_async_remote_copy(
        src_ref=src, dst_ref=dst, send_sem=send, recv_sem=recv, device_id=where, device_id_type=MESH
    )


def arrived(ref, sem):
    pltpu.make_async_copy(ref, ref, sem).wait()


def slot_shift(s):
    return jnp.where(s % 2 == 1, (s + 1) // 2, (NZ - s // 2) % NZ)


def kernel(
    feat, c_w, c_b, t_w, t_b, q_w, c_own, user, target,
    out, loss_out,
    a1, a2, w, t, cur1, cur2, part, mine, rs, hop, summed, cands, logits, u_own, loss,
    w_l, t_l, u_l,
    a2a_s, a2a_r, ag1_s, ag1_r, ag1_ls, ag2_s, ag2_r, ag2_ls, ag2_lr,
    z_s, z_r, y_s, y_r, l_s, l_r, da_s, da_r, db_s, db_r, dy_s, dy_r,
    t_s, t_r, td_s, td_r, c_s, c_r, rs_s, rs_r, hop_r, o_s, o_r, g_s, g_r,
):
    x = lax.axis_index("batch_1")
    y = lax.axis_index("batch_0")
    z = lax.axis_index("dim")
    c = lax.axis_index("field")
    p = x % 2
    wide = x // 2
    tall = 1 - wide
    xr, xl = (x + 1) % NX, (x + NX - 1) % NX
    yr, yl = (y + 1) % NX, (y + NX - 1) % NX
    zr, zl = (z + 1) % NZ, (z + NZ - 1) % NZ
    first = 2 * (1 - c)

    def lanes(j):
        return pl.ds(pl.multiple_of(j * 128, 128), 128)

    def ycols(who):
        return pl.ds(pl.multiple_of(who * KA, 128), KA)

    rest = pl.ds(NX * NY * 128, KR)

    barrier = pltpu.get_barrier_semaphore()

    def greet(where):
        pl.semaphore_signal(barrier, inc=1, device_id=where, device_id_type=MESH)

    for step in range(1, NX):
        for core in range(2):
            greet({"batch_1": (x + step) % NX, "field": core})
        greet({"batch_0": (y + step) % NX})
    for step in range(1, NZ):
        for core in range(2):
            greet({"dim": (z + step) % NZ, "field": core})
    greet({"field": 1 - c})

    base = HALF * wide + 6 * p
    own_w = [(level, k) for level in range(2) for k in range(NY + NREST - 1)]

    def own_copy(level, k):
        field = NY * y + k if k < NY else NX * NY + k - NY
        return pltpu.make_async_copy(
            c_w.at[level, pl.ds(6 * p, BLK), field], w.at[level, :, z, :, lanes(field)], w_l.at[level, k]
        )

    @pl.when(c == wide)
    def _():
        for level, k in own_w:
            own_copy(level, k).start()

    t_copies = [
        pltpu.make_async_copy(t_w.at[base + k], t.at[z, c, :, pl.ds(128 * k, 128)], t_l.at[k])
        for k in range(BLK)
    ]
    for cp in t_copies:
        cp.start()

    u_copy = pltpu.make_async_copy(user.at[pl.ds(pl.multiple_of(128 * z, 128), 128)], u_own, u_l)

    @pl.when(c == tall)
    def _():
        u_copy.start()

    row = lax.broadcasted_iota(jnp.int32, (NZ, SUB, 256), 0) * SUB + lax.broadcasted_iota(
        jnp.int32, (NZ, SUB, 256), 1
    )
    ones = jnp.where(row < 3, 1.0, 0.0).astype(BF16)
    a1[FIELDS] = ones
    a2[FIELDS] = ones

    def bias_block(values):
        n = values.shape[1]
        eye = lax.broadcasted_iota(jnp.int32, (n, n), 0) == lax.broadcasted_iota(jnp.int32, (n, n), 1)
        col = jnp.sum(jnp.where(eye, values, 0.0), axis=1, keepdims=True)
        hi = col.astype(BF16).astype(F32)
        mid = (col - hi).astype(BF16).astype(F32)
        low = (col - hi) - mid
        lane = lax.broadcasted_iota(jnp.int32, (n, 128), 1)
        terms = jnp.where(lane == 0, hi, jnp.where(lane == 1, mid, jnp.where(lane == 2, low, 0.0)))
        return terms.astype(BF16)

    t[z, c, :, BLK * 128 : BLK * 128 + 128] = q_w[...]
    t[z, c, :, BLK * 128 + 128 :] = bias_block(t_b[...])

    @pl.when(c == wide)
    def _():
        @pl.loop(0, BLK)
        def _(f):
            for level in range(2):
                w[level, f, z, :, FIELDS * 128 :] = bias_block(c_b[6 * p + f, level : level + 1])

        for level, k in own_w:
            own_copy(level, k).wait()

    @pl.when(c == tall)
    def _():
        a1[pl.ds(HALF * c, HALF), z, :, lanes(p)] = feat[:, :, lanes(z)]
        cands[NX * y + x] = c_own[...]

    for cp in t_copies:
        cp.wait()
    lane64 = lax.broadcasted_iota(jnp.int32, (64, 128), 1)
    edge = lanes((BLK - 1) * (1 - p))
    kept = (lane64 < 64) == (p == 0)
    t[z, c, :, edge] = jnp.where(kept, t[z, c, :, edge].astype(F32), 0.0).astype(BF16)

    pl.semaphore_wait(barrier, 3 * NX - 3 + 2 * NZ - 2 + 1)

    def examples_out(low, high):
        @pl.loop(low, high)
        def _(s):
            to = (z + slot_shift(s)) % NZ
            copy(
                feat.at[:, :, lanes(to)],
                a1.at[pl.ds(HALF * c, HALF), z, :, lanes(p)],
                a2a_s.at[0], a2a_r.at[slot_shift(s)], {"dim": to, "field": tall},
            ).start()

    def along_z(ref, level, s, k, d):
        to = jnp.where(d == 0, zr, zl)
        nxt = jnp.where(s == 0, 1 + d, jnp.minimum(s + 2, NZ - 1))
        copy(ref, ref, z_s.at[level, d, k], z_r.at[level, nxt, k], {"dim": to}).start()

    def hand_over(level, s):
        ref = w.at[level, :, (z + NZ - slot_shift(s)) % NZ, :, ycols(y)]
        copy(ref, ref, da_s.at[level], da_r.at[level, s], {"field": 1 - c}).start()

    def from_z(level, s, k):
        src = (z + NZ - slot_shift(s)) % NZ
        ref = w.at[level, :, src, :, rest] if k else w.at[level, :, src, :, ycols(y)]
        onward = ((s < 5) | (s == 6)) if k else (s < 6)

        @pl.when(s > 0)
        def _():
            arrived(ref, z_r.at[level, s, k])

        @pl.when((s > 0) & onward)
        def _():
            along_z(ref, level, s, k, jnp.where(s % 2 == 1, 0, 1))

        @pl.when(s == 0)
        def _():
            along_z(ref, level, s, k, 0)
            along_z(ref, level, s, k, 1)

        if k:
            copy(ref, ref, db_s.at[level], db_r.at[level, s], {"field": 1 - c}).start()
        elif level == 0:
            hand_over(level, s)
        else:
            @pl.when(s > 0)
            def _():
                hand_over(level, s)

    def from_a(level, s):
        from_z(level, s, 0)

    def from_b(level, s):
        from_z(level, s, 1)

    def to_y(level, s):
        src = (z + NZ - slot_shift(s)) % NZ
        own = w.at[level, :, src, :, ycols(y)]
        arrived(own, da_r.at[level, s])
        copy(own, own, y_s.at[level, 0], y_r.at[level, s, 0], {"batch_0": yr}).start()
        copy(own, own, y_s.at[level, 1], y_r.at[level, s, 1], {"batch_0": yl}).start()

    def from_y(level, s):
        src = (z + NZ - slot_shift(s)) % NZ
        left = w.at[level, :, src, :, ycols(yl)]
        right = w.at[level, :, src, :, ycols(yr)]
        up = w.at[level, pl.ds(0, 4), src, :, ycols(yl)]
        down = w.at[level, pl.ds(4, 3), src, :, ycols(yr)]
        arrived(left, y_r.at[level, s, 0])
        copy(up, up, l_s.at[level, 0], l_r.at[level, s, 0], {"batch_0": yr}).start()
        copy(left, left, dy_s.at[level], dy_r.at[level, s], {"field": 1 - c}).start()
        arrived(right, y_r.at[level, s, 1])
        copy(down, down, l_s.at[level, 1], l_r.at[level, s, 1], {"batch_0": yl}).start()
        copy(right, right, dy_s.at[level], dy_r.at[level, s], {"field": 1 - c}).start()

    def to_core(level, s):
        src = (z + NZ - slot_shift(s)) % NZ
        far = (y + 2) % NX
        piece = w.at[level, :, src, :, ycols(far)]
        arrived(w.at[level, pl.ds(0, 4), src, :, ycols(far)], l_r.at[level, s, 0])
        arrived(w.at[level, pl.ds(4, 3), src, :, ycols(far)], l_r.at[level, s, 1])
        copy(piece, piece, dy_s.at[level], dy_r.at[level, s], {"field": 1 - c}).start()

    def tower_step(s):
        src = (z + NZ - slot_shift(s)) % NZ
        whole = t.at[src, c]

        @pl.when(s == 0)
        def _():
            copy(whole, whole, t_s.at[0], t_r.at[1], {"dim": zr}).start()
            copy(whole, whole, t_s.at[1], t_r.at[2], {"dim": zl}).start()

        @pl.when((s > 0) & (s < 7))
        def _():
            arrived(whole, t_r.at[s])

        for par, to in ((1, zr), (0, zl)):
            d = 1 - par
            half = t.at[src, c, pl.ds(32 * d, 32)]

            @pl.when((s > 0) & (s < 5) & (s % 2 == par))
            def _():
                copy(whole, whole, t_s.at[d], t_r.at[s + 2], {"dim": to}).start()

            @pl.when(s == 6 - par)
            def _():
                copy(half, half, t_s.at[2 + d], t_r.at[7 + d], {"dim": to}).start()

        @pl.when(s == 7)
        def _():
            arrived(t.at[src, c, pl.ds(0, 32)], t_r.at[7])
            arrived(t.at[src, c, pl.ds(32, 32)], t_r.at[8])

        copy(whole, whole, td_s, td_r, {"field": 1 - c}).start()

    def example_step(s):
        dz = slot_shift(s)
        src = (z + NZ - dz) % NZ
        whole = a1.at[pl.ds(0, FIELDS), src, :, lanes(p)]

        @pl.when(s == 0)
        def _():
            arrived(a1.at[pl.ds(0, HALF), src, :, lanes(p)], a2a_r.at[0])

        @pl.when(s > 0)
        def _():
            arrived(whole, a2a_r.at[dz])

        copy(whole, whole, ag1_s.at[0], ag1_r.at[p, s, 0], {"batch_1": xr}).start()
        copy(whole, whole, ag1_s.at[1], ag1_r.at[p, s, 1], {"batch_1": xl}).start()

    def relay_step(s):
        src = (z + NZ - slot_shift(s)) % NZ
        for j in range(2):
            r = (x + NX - first - j) % NX
            whole = a1.at[pl.ds(0, FIELDS), src, :, pl.ds(128 * j, 128)]

            @pl.when(r == 1)
            def _():
                arrived(whole, ag1_r.at[j, s, 0])
                half = a1.at[pl.ds(0, HALF), src, :, pl.ds(128 * j, 128)]
                copy(half, half, ag1_ls.at[0], ag1_r.at[j, s, 0], {"batch_1": xr}).start()

            @pl.when(r == 3)
            def _():
                arrived(whole, ag1_r.at[j, s, 1])
                half = a1.at[pl.ds(HALF, HALF), src, :, pl.ds(128 * j, 128)]
                copy(half, half, ag1_ls.at[1], ag1_r.at[j, s, 1], {"batch_1": xl}).start()

    def far_step(s):
        src = (z + NZ - slot_shift(s)) % NZ
        for j in range(2):
            r = (x + NX - first - j) % NX

            @pl.when(r == 2)
            def _():
                arrived(a1.at[pl.ds(0, HALF), src, :, pl.ds(128 * j, 128)], ag1_r.at[j, s, 0])
                arrived(a1.at[pl.ds(HALF, HALF), src, :, pl.ds(128 * j, 128)], ag1_r.at[j, s, 1])

    def owned(ref, field, s, extra):
        src = (z + NZ - slot_shift(s)) % NZ
        return ref.at[pl.ds(field, 1 if extra else 6), src]

    def with_extra(who, s, act):
        act(13 * (who // 2) + 7 * (who % 2), False)

        @pl.when(((z + NZ - slot_shift(s)) % NZ) // 4 == who % 2)
        def _():
            act(13 * (who // 2) + 6, True)

    def second_send(s):
        def act(field, extra):
            kind = 1 if extra else 0
            mineh = owned(cur1, field - base, s, extra)
            there = owned(a2, field, s, extra)
            copy(mineh, there, ag2_s.at[kind, 0], ag2_r.at[kind, s, 0], {"batch_1": xr}).start()
            copy(mineh, there, ag2_s.at[kind, 1], ag2_r.at[kind, s, 1], {"batch_1": xl}).start()
            there[...] = mineh[...]

        with_extra(x, s, act)

    def second_step(s):
        for d, who, to in ((0, xl, xr), (1, xr, xl)):
            def act(field, extra):
                kind = 1 if extra else 0
                piece = owned(a2, field, s, extra)
                arrived(piece, ag2_r.at[kind, s, d])

                @pl.when((z + NZ - slot_shift(s)) % 2 == 1 - d)
                def _():
                    copy(piece, piece, ag2_ls.at[kind, d], ag2_lr.at[kind, s], {"batch_1": to}).start()

            with_extra(who, s, act)

    def second_far(s):
        def act(field, extra):
            arrived(owned(a2, field, s, extra), ag2_lr.at[1 if extra else 0, s])

        with_extra((x + 2) % NX, s, act)

    def crossed(to):
        for j in range(2):
            where = {"batch_1": first + j, "dim": to, "field": wide}
            copy(
                cur2.at[pl.ds(p, 6), to, :, lanes(j)],
                out.at[pl.ds(7 * p, 6), :, lanes(z)],
                o_s.at[0], o_r, where,
            ).start()

            @pl.when((to // 4) == p)
            def _():
                copy(
                    cur2.at[pl.ds(6 - 6 * p, 1), to, :, lanes(j)],
                    out.at[pl.ds(6, 1), :, lanes(z)],
                    o_s.at[1], o_r, where,
                ).start()

    def layer(level, s):
        src = (z + NZ - slot_shift(s)) % NZ
        lhs = w[level, :, src].reshape(BLK * SUB, KW)
        anchor = a1[pl.ds(base, BLK), src].reshape(BLK * SUB, 256).astype(F32)
        if level == 0:
            rhs = a1[...].reshape(KW, 256)
            before = anchor
        else:
            rhs = a2[...].reshape(KW, 256)
            before = cur1[:, src].reshape(BLK * SUB, 256).astype(F32)
        prod = jnp.dot(lhs, rhs, preferred_element_type=F32)
        nxt = (anchor * prod + before).astype(BF16).reshape(BLK, SUB, 256)
        if level == 0:
            cur1[:, src] = nxt
            second_send(s)
        else:
            cur2[:, src] = nxt
            crossed(src)

    def rows_here(level, s):
        src = (z + NZ - slot_shift(s)) % NZ

        @pl.when(c == wide)
        def _():
            arrived(w.at[level, :, src, :, pl.ds(0, 3 * KA)], dy_r.at[level, s])

        @pl.when(c == tall)
        def _():
            arrived(w.at[level, :, src, :, rest], db_r.at[level, s])

    @pl.when(c == wide)
    def _():
        from_a(0, 0)
        copy(
            feat.at[:, :, lanes(z)],
            a1.at[pl.ds(HALF * c, HALF), z, :, lanes(p)],
            a2a_s.at[1], a2a_r.at[0], {"field": tall},
        ).start()
        hand_over(1, 0)
        examples_out(1, 3)

        @pl.loop(1, 14)
        def _(i):
            @pl.when(i < NZ)
            def _():
                from_a(0, i)

            for due, low, high in ((2, 3, 5), (4, 5, 7), (5, 7, 8)):
                @pl.when(i == due)
                def _():
                    examples_out(low, high)

            @pl.when((i >= 4) & (i < 12))
            def _():
                from_b(0, i - 4)

            @pl.when(i >= 6)
            def _():
                from_a(1, i - 6)

            @pl.when((i >= 5) & (i < 13))
            def _():
                relay_step(i - 5)

            @pl.when(i == 10)
            def _():
                tower_step(0)

            @pl.when(i >= 11)
            def _():
                from_b(1, i - 11)

        tower_step(1)
        tower_step(2)

        @pl.loop(0, NZ)
        def _(i):
            far_step(i)

        @pl.loop(0, NZ)
        def _(s):
            rows_here(0, s)
            layer(0, s)

    @pl.when(c == tall)
    def _():
        examples_out(1, 3)
        to_y(0, 0)
        to_y(1, 0)
        for step in range(1, NX):
            to = (x + step) % NX
            copy(
                c_own, cands.at[NX * y + x], c_s.at[0], c_r.at[0], {"batch_1": to, "field": 1 - to // 2}
            ).start()
        example_step(0)
        from_y(0, 0)

        @pl.loop(1, 12)
        def _(i):
            @pl.when(i < NZ)
            def _():
                to_y(0, i)

            for due in (1, 2, 3):
                @pl.when(i == due)
                def _():
                    examples_out(2 * due + 1, min(2 * due + 3, NZ))

            @pl.when(i == 1)
            def _():
                from_y(1, 0)

            @pl.when((i > 1) & (i < NZ + 1))
            def _():
                from_y(0, i - 1)

            @pl.when((i > 1) & (i < NZ + 1))
            def _():
                example_step(i - 1)

            @pl.when(i >= 8)
            def _():
                to_y(1, i - 7)

            @pl.when(i >= 10)
            def _():
                from_y(1, i - 9)

            @pl.when(i == 11)
            def _():
                @pl.loop(5, NZ)
                def _(s):
                    to_y(1, s)

            @pl.when((i >= 3) & (i < 11))
            def _():
                to_core(0, i - 3)

            @pl.when((i >= 3) & (i < 11))
            def _():
                relay_step(i - 3)

            @pl.when(i == 4)
            def _():
                to_core(1, 0)

            @pl.when(i == 8)
            def _():
                tower_step(0)

            @pl.when(i == 11)
            def _():
                tower_step(1)
                tower_step(2)

            @pl.when(i >= 10)
            def _():
                @pl.loop(0, 3)
                def _(k):
                    s = 3 * (i - 10) + k
                    rows_here(0, s)
                    layer(0, s)

        @pl.loop(6, NZ)
        def _(s):
            rows_here(0, s)
            layer(0, s)

    @pl.when(c == wide)
    def _():
        @pl.loop(0, NZ)
        def _(i):
            @pl.when((i % 4 == 0) | (i % 4 == 1))
            def _():
                k = 3 + 2 * (i // 4) + i % 4
                from_b(1, k)
                tower_step(k)

            second_step(i)

        from_b(1, 7)
        tower_step(7)

    @pl.when(c == tall)
    def _():
        @pl.loop(5, 10)
        def _(i):
            from_y(1, i - 2)
            to_core(1, i - 4)

            @pl.when(i < 9)
            def _():
                second_step(2 * i - 10)
                second_step(2 * i - 9)

            @pl.when(i >= 6)
            def _():
                tower_step(i - 3)

        to_core(1, 6)
        tower_step(7)

    @pl.loop(0, NZ)
    def _(s):
        second_far(s)

    @pl.loop(0, NZ)
    def _(s):
        @pl.when((c == tall) & (s == 4))
        def _():
            to_core(1, 7)
            got = cands.at[pl.ds(NX * y, NX)]
            arrived(cands.at[pl.ds(NX * y, NX - 1)], c_r.at[0])
            for step in range(1, NX):
                copy(got, got, c_s.at[1], c_r.at[1], {"batch_0": (y + step) % NX}).start()

        rows_here(1, s)
        layer(1, s)

    arrived(t.at[:, c], td_r)

    def tower(k):
        lhs = t[k, :, :, 0 : BLK * 128].reshape(128, BLK * 128)
        prod = jnp.dot(lhs, cur2[...].reshape(BLK * 128, 256), preferred_element_type=F32)
        part[pl.ds(128 * k, 128)] = prod.astype(BF16)
        mine[pl.ds(128 * k, 128)] = prod

    def far_sum(h):
        for j in range(2):
            @pl.when((x + NX - first - j) % NX == 2)
            def _():
                to = (xr, xl)[h]
                copy(
                    part.at[pl.ds(512 * h, 512), pl.ds(128 * j, 128)], hop, rs_s.at[h], hop_r, {"batch_1": to}
                ).start()

    for h in range(2):
        @pl.loop(4 * h, 4 * h + 4)
        def _(k):
            tower(k)

        far_sum(h)

    for r, own, added, way in ((1, 0, 512, xl), (3, 512, 0, xr)):
        for j in range(2):
            @pl.when((x + NX - first - j) % NX == r)
            def _():
                cols = pl.ds(128 * j, 128)
                slot = rs.at[r // 2]
                copy(
                    part.at[pl.ds(own, 512), cols], slot.at[pl.ds(own, 512)], rs_s.at[2], rs_r, {"batch_1": way}
                ).start()
                arrived(hop, hop_r)
                summed[...] = (mine[pl.ds(added, 512), cols] + hop[...].astype(F32)).astype(BF16)
                copy(summed, slot.at[pl.ds(added, 512)], rs_s.at[3], rs_r, {"batch_1": way}).start()

    @pl.when(c == tall)
    def _():
        arrived(rs, rs_r)

    for j in range(2):
        r = (x + NX - first - j) % NX

        @pl.when(r == 2)
        def _():
            arrived(hop, rs_s.at[0])
            arrived(hop, rs_s.at[1])

        @pl.when((r == 1) | (r == 3))
        def _():
            arrived(hop, rs_s.at[2])
            arrived(hop, rs_s.at[3])

    @pl.when(c == tall)
    def _():
        here = lanes(p)
        bias = t[:, :, :, BLK * 128 + 128 :].reshape(UNITS, 128).astype(F32)
        bias = bias[:, 0:1] + bias[:, 1:2] + bias[:, 2:3]
        total = mine[:, here] + rs[0].astype(F32) + rs[1].astype(F32)
        hidden = jnp.maximum(total + bias, 0.0).astype(BF16)
        qw = t[:, :, :, BLK * 128 : BLK * 128 + 128].reshape(UNITS, 128)
        query = lax.dot_general(qw, hidden, (((0,), (0,)), ((), ())), preferred_element_type=F32)
        u_copy.wait()
        query = (query + u_own[...].astype(F32).T).astype(BF16)

        arrived(cands.at[pl.ds(0, 3 * NX)], c_r.at[1])
        scale = 1.0 / math.sqrt(128)

        def scores(k, top):
            got = jnp.dot(cands[k], query, preferred_element_type=F32) * scale
            logits[k] = got
            return jnp.maximum(top, jnp.max(got.reshape(32, 8, 128), axis=0))

        top = lax.fori_loop(0, NX * NX, scores, jnp.full((8, 128), -1e30, F32), unroll=4)
        top = jnp.max(top, axis=0, keepdims=True)
        wanted = target[pl.ds(z, 1), :]
        index = lax.broadcasted_iota(jnp.int32, (256, 128), 0)

        def sums(k, carry):
            total, picked = carry
            got = logits[k]
            e = jnp.exp(got - top)
            hit = jnp.where(index == wanted - 256 * k, got, 0.0)
            return (
                total + jnp.sum(e.reshape(32, 8, 128), axis=0),
                picked + jnp.sum(hit.reshape(32, 8, 128), axis=0),
            )

        zero = jnp.zeros((8, 128), F32)
        total, picked = lax.fori_loop(0, NX * NX, sums, (zero, zero), unroll=4)
        total = jnp.sum(total, axis=0, keepdims=True)
        picked = jnp.sum(picked, axis=0, keepdims=True)
        result = top + jnp.log(total) - picked
        loss[z] = jnp.broadcast_to(result, (8, 128))

        @pl.loop(1, NZ)
        def _(dz):
            to = (z + dz) % NZ
            copy(loss.at[z], loss.at[z], g_s.at[0], g_r, {"dim": to}).start()
            copy(loss.at[z], loss.at[z], g_s.at[1], g_r, {"dim": to, "field": wide}).start()

        copy(loss.at[z], loss.at[z], g_s.at[2], g_r, {"field": wide}).start()
        arrived(loss.at[pl.ds(0, NZ - 1)], g_r)
        arrived(loss.at[pl.ds(0, NZ - 1)], g_s.at[0])
        arrived(loss.at[pl.ds(0, NZ - 1)], g_s.at[1])
        arrived(loss.at[0], g_s.at[2])
        arrived(cands.at[pl.ds(0, 3)], c_s.at[0])
        arrived(cands.at[pl.ds(0, 3 * NX)], c_s.at[1])
        for d in range(2):
            arrived(a1.at[pl.ds(0, FIELDS), :, :, pl.ds(0, 128)], ag1_s.at[d])
        for level in range(2):
            for d in range(2):
                arrived(w.at[level, :, :, :, pl.ds(0, KA)], y_s.at[level, d])
            arrived(w.at[level, pl.ds(0, 4), :, :, pl.ds(0, KA)], l_s.at[level, 0])
            arrived(w.at[level, pl.ds(4, 3), :, :, pl.ds(0, KA)], l_s.at[level, 1])
            arrived(w.at[level, :, :, :, pl.ds(0, 3 * KA)], dy_s.at[level])

    @pl.when(c == wide)
    def _():
        arrived(loss, g_r)
        arrived(feat.at[:, :, pl.ds(0, 128)], a2a_s.at[1])
        for level in range(2):
            arrived(w.at[level, :, pl.ds(0, 4), :, pl.ds(0, KA)], z_s.at[level, 0, 0])
            arrived(w.at[level, :, pl.ds(0, 3), :, pl.ds(0, KA)], z_s.at[level, 1, 0])
            arrived(w.at[level, :, pl.ds(0, 3), :, rest], z_s.at[level, 0, 1])
            arrived(w.at[level, :, pl.ds(0, 4), :, rest], z_s.at[level, 1, 1])
            arrived(w.at[level, :, :, :, pl.ds(0, KA)], da_s.at[level])
            arrived(w.at[level, :, :, :, rest], db_s.at[level])

    arrived(feat.at[:, :, pl.ds(0, 128 * (NZ - 1))], a2a_s.at[0])
    for j in range(2):
        r = (x + NX - first - j) % NX

        @pl.when(r == 1)
        def _():
            arrived(a1.at[pl.ds(0, HALF), :, :, pl.ds(0, 128)], ag1_ls.at[0])

        @pl.when(r == 3)
        def _():
            arrived(a1.at[pl.ds(0, HALF), :, :, pl.ds(0, 128)], ag1_ls.at[1])

    for d in range(2):
        arrived(a2.at[pl.ds(0, 6)], ag2_s.at[0, d])
        arrived(a2.at[0, pl.ds(0, 4)], ag2_s.at[1, d])
        arrived(a2.at[pl.ds(0, 6), pl.ds(0, 4)], ag2_ls.at[0, d])
        arrived(a2.at[0, pl.ds(0, 2)], ag2_ls.at[1, d])
    for d in range(2):
        arrived(t.at[pl.ds(0, 3), 0], t_s.at[d])
        arrived(t.at[0, 0, pl.ds(0, 32)], t_s.at[2 + d])
    arrived(t.at[:, 0], td_s)
    arrived(cur2.at[pl.ds(0, 6)], o_s.at[0])
    arrived(cur2.at[0, pl.ds(0, 4)], o_s.at[1])
    for k in range(NZ):
        loss_out[k : k + 1] = loss[k, 0:1]
    arrived(out, o_r)


def body(features, cross_weight, cross_bias, tower_weight, tower_bias, query_weight, user_vec, candidates, positive):
    vmem = pl.BlockSpec(memory_space=pltpu.VMEM)
    hbm = pl.BlockSpec(memory_space=pl.ANY)
    dma = pltpu.SemaphoreType.DMA
    out, loss = pl.pallas_call(
        kernel,
        out_shape=(
            pltpu.VMEM((HALF, SUB, 1024), BF16),
            pltpu.VMEM((NZ, 128), F32),
        ),
        in_specs=[vmem, hbm, vmem, hbm, vmem, vmem, vmem, hbm, vmem],
        out_specs=(vmem, vmem),
        scratch_shapes=[
            pltpu.VMEM((KB, NZ, SUB, 256), BF16),
            pltpu.VMEM((KB, NZ, SUB, 256), BF16),
            pltpu.VMEM((2, BLK, NZ, SUB, KW), BF16),
            pltpu.VMEM((NZ, 2, 64, TC), BF16),
            pltpu.VMEM((BLK, NZ, SUB, 256), BF16),
            pltpu.VMEM((BLK, NZ, SUB, 256), BF16),
            pltpu.VMEM((UNITS, 256), BF16),
            pltpu.VMEM((UNITS, 256), F32),
            pltpu.VMEM((2, UNITS, 128), BF16),
            pltpu.VMEM((UNITS // 2, 128), BF16),
            pltpu.VMEM((UNITS // 2, 128), BF16),
            pltpu.VMEM((NX * NX, 256, 128), BF16),
            pltpu.VMEM((NX * NX, 256, 128), F32),
            pltpu.VMEM((128, 128), BF16),
            pltpu.VMEM((NZ, 8, 128), F32),
            dma((2, NY + NREST - 1)), dma((BLK,)), dma,
            dma((2,)), dma((NZ,)),
            dma((2,)), dma((2, NZ, 2)), dma((2,)),
            dma((2, 2)), dma((2, NZ, 2)), dma((2, 2)), dma((2, NZ)),
            dma((2, 2, 2)), dma((2, NZ, 2)),
            dma((2, 2)), dma((2, NZ, 2)),
            dma((2, 2)), dma((2, NZ, 2)),
            dma((2,)), dma((2, NZ)), dma((2,)), dma((2, NZ)), dma((2,)), dma((2, NZ)),
            dma((4,)), dma((9,)), dma, dma,
            dma((2,)), dma((2,)),
            dma((4,)), dma, dma,
            dma((2,)), dma,
            dma((3,)), dma,
        ],
        compiler_params=pltpu.CompilerParams(collective_id=0, has_side_effects=True, vmem_limit_bytes=60 * 1024 * 1024),
        name="dcn",
    )(
        features,
        cross_weight.transpose(0, 1, 3, 2, 4),
        cross_bias.transpose(1, 0, 2),
        tower_weight.transpose(1, 0, 2),
        tower_bias.reshape(1, 64),
        query_weight,
        candidates,
        user_vec,
        positive.reshape(NZ, 128),
    )
    return out, loss.reshape(1024)


def solution(mesh):
    torus = Mesh(
        mesh.devices.reshape(4, 4, mesh.shape["field"], mesh.shape["dim"]),
        ("batch_0", "batch_1", "field", "dim"),
    )
    in_specs = (
        P("field", "dim", BATCH),
        P(None, "field", "dim", None, None),
        P(None, "field", "dim"),
        P(("field", "dim"), None, None),
        P(("field", "dim")),
        P(("field", "dim"), None),
        P(BATCH, None),
        P(BATCH, None),
        P(BATCH),
    )
    out_specs = (P("field", "dim", BATCH), P(BATCH))
    return jax.shard_map(body, mesh=torus, in_specs=in_specs, out_specs=out_specs, check_vma=False)
```

```python
import functools
import math

import jax
import jax.numpy as jnp
from jax import lax
from jax.experimental import pallas as pl
from jax.experimental.pallas import tpu as pltpu
from jax.sharding import Mesh
from jax.sharding import PartitionSpec as P

BATCH = ("batch_0", "batch_1")
MESH = pl.DeviceIdType.MESH
F32 = jnp.float32
BF16 = jnp.bfloat16

FIELDS = 26
NX = 4
NZ = 8
HALF = 13
SUB = 16
BLK = 7
NY = 6
NREST = FIELDS + 1 - NX * NY
KB = FIELDS + 1
KA = NY * 128
KR = NREST * 128
KW = KB * 128
GROUP = 2
TC = BLK * 128 + 256
UNITS = 1024


def copy(src, dst, send, recv, where):
    return pltpu.make_async_remote_copy(
        src_ref=src, dst_ref=dst, send_sem=send, recv_sem=recv, device_id=where, device_id_type=MESH
    )


def arrived(ref, sem):
    pltpu.make_async_copy(ref, ref, sem).wait()


def slot_shift(s):
    return jnp.where(s % 2 == 1, (s + 1) // 2, (NZ - s // 2) % NZ)


def kernel(
    feat, c_w, c_b, t_w, t_b, q_w, c_own, user, target,
    out, loss_out,
    a1, a2, w, t, cur1, cur2, part, mine, rs, hop, summed, cands, logits, u_own, loss,
    w_l, t_l, u_l,
    a2a_s, a2a_r, ag1_s, ag1_r, ag1_ls, ag2_s, ag2_r, ag2_ls, ag2_lr,
    z_s, z_r, y_s, y_r, l_s, l_r, da_s, da_r, db_s, db_r, dy_s, dy_r,
    t_s, t_r, td_s, td_r, c_s, c_r, rs_s, rs_r, hop_r, o_s, o_r, g_s, g_r,
):
    x = lax.axis_index("batch_1")
    y = lax.axis_index("batch_0")
    z = lax.axis_index("dim")
    c = lax.axis_index("field")
    p = x % 2
    wide = x // 2
    tall = 1 - wide
    xr, xl = (x + 1) % NX, (x + NX - 1) % NX
    yr, yl = (y + 1) % NX, (y + NX - 1) % NX
    zr, zl = (z + 1) % NZ, (z + NZ - 1) % NZ
    first = 2 * (1 - c)

    def lanes(j):
        return pl.ds(pl.multiple_of(j * 128, 128), 128)

    def ycols(who):
        return pl.ds(pl.multiple_of(who * KA, 128), KA)

    rest = pl.ds(NX * NY * 128, KR)

    barrier = pltpu.get_barrier_semaphore()

    def greet(where):
        pl.semaphore_signal(barrier, inc=1, device_id=where, device_id_type=MESH)

    for step in range(1, NX):
        for core in range(2):
            greet({"batch_1": (x + step) % NX, "field": core})
        greet({"batch_0": (y + step) % NX})
    for step in range(1, NZ):
        for core in range(2):
            greet({"dim": (z + step) % NZ, "field": core})
    greet({"field": 1 - c})

    base = HALF * wide + 6 * p
    own_w = [(level, k) for level in range(2) for k in range(NY + NREST - 1)]

    def own_copy(level, k):
        field = NY * y + k if k < NY else NX * NY + k - NY
        return pltpu.make_async_copy(
            c_w.at[level, pl.ds(6 * p, BLK), field], w.at[level, :, z, :, lanes(field)], w_l.at[level]
        )

    @pl.when(c == wide)
    def _():
        for level, k in own_w:
            own_copy(level, k).start()

    t_copies = [
        pltpu.make_async_copy(t_w.at[base + k], t.at[z, c, :, pl.ds(128 * k, 128)], t_l)
        for k in range(BLK)
    ]
    for cp in t_copies:
        cp.start()

    u_copy = pltpu.make_async_copy(user.at[pl.ds(pl.multiple_of(128 * z, 128), 128)], u_own, u_l)

    @pl.when(c == tall)
    def _():
        u_copy.start()

    row = lax.broadcasted_iota(jnp.int32, (NZ, SUB, 256), 0) * SUB + lax.broadcasted_iota(
        jnp.int32, (NZ, SUB, 256), 1
    )
    ones = jnp.where(row < 3, 1.0, 0.0).astype(BF16)
    a1[FIELDS] = ones
    a2[FIELDS] = ones

    def bias_block(values):
        n = values.shape[1]
        eye = lax.broadcasted_iota(jnp.int32, (n, n), 0) == lax.broadcasted_iota(jnp.int32, (n, n), 1)
        col = jnp.sum(jnp.where(eye, values, 0.0), axis=1, keepdims=True)
        hi = col.astype(BF16).astype(F32)
        mid = (col - hi).astype(BF16).astype(F32)
        low = (col - hi) - mid
        lane = lax.broadcasted_iota(jnp.int32, (n, 128), 1)
        terms = jnp.where(lane == 0, hi, jnp.where(lane == 1, mid, jnp.where(lane == 2, low, 0.0)))
        return terms.astype(BF16)

    t[z, c, :, BLK * 128 : BLK * 128 + 128] = q_w[...]
    t[z, c, :, BLK * 128 + 128 :] = bias_block(t_b[...])

    @pl.when(c == wide)
    def _():
        @pl.loop(0, BLK)
        def _(f):
            for level in range(2):
                w[level, f, z, :, FIELDS * 128 :] = bias_block(c_b[6 * p + f, level : level + 1])

        for level in range(2):
            arrived(w.at[level, :, z, :, pl.ds(0, 128 * (NY + NREST - 1))], w_l.at[level])

    @pl.when(c == tall)
    def _():
        a1[pl.ds(HALF * c, HALF), z, :, lanes(p)] = feat[:, :, lanes(z)]
        cands[NX * y + x] = c_own[...]

    arrived(t.at[z, c, :, pl.ds(0, 128 * BLK)], t_l)
    lane64 = lax.broadcasted_iota(jnp.int32, (64, 128), 1)
    edge = lanes((BLK - 1) * (1 - p))
    kept = (lane64 < 64) == (p == 0)
    t[z, c, :, edge] = jnp.where(kept, t[z, c, :, edge].astype(F32), 0.0).astype(BF16)

    pl.semaphore_wait(barrier, 3 * NX - 3 + 2 * NZ - 2 + 1)

    def examples_out(low, high):
        @pl.loop(low, high)
        def _(s):
            to = (z + slot_shift(s)) % NZ
            copy(
                feat.at[:, :, lanes(to)],
                a1.at[pl.ds(HALF * c, HALF), z, :, lanes(p)],
                a2a_s.at[0], a2a_r.at[slot_shift(s)], {"dim": to, "field": tall},
            ).start()

    def along_z(ref, level, s, k, d):
        to = jnp.where(d == 0, zr, zl)
        nxt = jnp.where(s == 0, 1 + d, jnp.minimum(s + 2, NZ - 1))
        copy(ref, ref, z_s.at[level, d, k], z_r.at[level, nxt, k], {"dim": to}).start()

    def hand_over(level, s):
        ref = w.at[level, :, (z + NZ - slot_shift(s)) % NZ, :, ycols(y)]
        copy(ref, ref, da_s.at[level], da_r.at[level, s], {"field": 1 - c}).start()

    def from_z(level, s, k):
        src = (z + NZ - slot_shift(s)) % NZ
        ref = w.at[level, :, src, :, rest] if k else w.at[level, :, src, :, ycols(y)]
        onward = ((s < 5) | (s == 6)) if k else (s < 6)

        @pl.when(s > 0)
        def _():
            arrived(ref, z_r.at[level, s, k])

        @pl.when((s > 0) & onward)
        def _():
            along_z(ref, level, s, k, jnp.where(s % 2 == 1, 0, 1))

        @pl.when(s == 0)
        def _():
            along_z(ref, level, s, k, 0)
            along_z(ref, level, s, k, 1)

        if k:
            copy(ref, ref, db_s.at[level], db_r.at[level], {"field": 1 - c}).start()
        elif level == 0:
            hand_over(level, s)
        else:
            @pl.when(s > 0)
            def _():
                hand_over(level, s)

    def from_a(level, s):
        from_z(level, s, 0)

    def from_b(level, s):
        from_z(level, s, 1)

    def to_y(level, s):
        src = (z + NZ - slot_shift(s)) % NZ
        own = w.at[level, :, src, :, ycols(y)]
        arrived(own, da_r.at[level, s])
        copy(own, own, y_s.at[level, 0], y_r.at[level, s, 0], {"batch_0": yr}).start()
        copy(own, own, y_s.at[level, 1], y_r.at[level, s, 1], {"batch_0": yl}).start()

    def from_y(level, s):
        src = (z + NZ - slot_shift(s)) % NZ
        left = w.at[level, :, src, :, ycols(yl)]
        right = w.at[level, :, src, :, ycols(yr)]
        up = w.at[level, pl.ds(0, 4), src, :, ycols(yl)]
        down = w.at[level, pl.ds(4, 3), src, :, ycols(yr)]
        arrived(left, y_r.at[level, s, 0])
        copy(up, up, l_s.at[level, 0], l_r.at[level, s], {"batch_0": yr}).start()
        copy(left, left, dy_s.at[level], dy_r.at[level, s], {"field": 1 - c}).start()
        arrived(right, y_r.at[level, s, 1])
        copy(down, down, l_s.at[level, 1], l_r.at[level, s], {"batch_0": yl}).start()
        copy(right, right, dy_s.at[level], dy_r.at[level, s], {"field": 1 - c}).start()

    def to_core(level, s):
        src = (z + NZ - slot_shift(s)) % NZ
        far = (y + 2) % NX
        piece = w.at[level, :, src, :, ycols(far)]
        arrived(piece, l_r.at[level, s])
        copy(piece, piece, dy_s.at[level], dy_r.at[level, s], {"field": 1 - c}).start()

    def tower_step(s):
        src = (z + NZ - slot_shift(s)) % NZ
        whole = t.at[src, c]

        @pl.when(s == 0)
        def _():
            copy(whole, whole, t_s.at[0], t_r.at[1], {"dim": zr}).start()
            copy(whole, whole, t_s.at[1], t_r.at[2], {"dim": zl}).start()

        @pl.when((s > 0) & (s < 7))
        def _():
            arrived(whole, t_r.at[s])

        for par, to in ((1, zr), (0, zl)):
            d = 1 - par
            half = t.at[src, c, pl.ds(32 * d, 32)]

            @pl.when((s > 0) & (s < 5) & (s % 2 == par))
            def _():
                copy(whole, whole, t_s.at[d], t_r.at[s + 2], {"dim": to}).start()

            @pl.when(s == 6 - par)
            def _():
                copy(half, half, t_s.at[2 + d], t_r.at[7 + d], {"dim": to}).start()

        @pl.when(s == 7)
        def _():
            arrived(t.at[src, c, pl.ds(0, 32)], t_r.at[7])
            arrived(t.at[src, c, pl.ds(32, 32)], t_r.at[8])

        copy(whole, whole, td_s, td_r, {"field": 1 - c}).start()

    def example_step(s):
        dz = slot_shift(s)
        src = (z + NZ - dz) % NZ
        whole = a1.at[pl.ds(0, FIELDS), src, :, lanes(p)]

        @pl.when(s == 0)
        def _():
            arrived(a1.at[pl.ds(0, HALF), src, :, lanes(p)], a2a_r.at[0])

        @pl.when(s > 0)
        def _():
            arrived(whole, a2a_r.at[dz])

        copy(whole, whole, ag1_s.at[0], ag1_r.at[p, s], {"batch_1": xr}).start()
        copy(whole, whole, ag1_s.at[1], ag1_r.at[p, s], {"batch_1": xl}).start()

    def relay_step(s):
        src = (z + NZ - slot_shift(s)) % NZ
        for j in range(2):
            r = (x + NX - first - j) % NX
            whole = a1.at[pl.ds(0, FIELDS), src, :, pl.ds(128 * j, 128)]

            @pl.when(r == 1)
            def _():
                arrived(whole, ag1_r.at[j, s])
                half = a1.at[pl.ds(0, HALF), src, :, pl.ds(128 * j, 128)]
                copy(half, half, ag1_ls.at[0], ag1_r.at[j, s], {"batch_1": xr}).start()

            @pl.when(r == 3)
            def _():
                arrived(whole, ag1_r.at[j, s])
                half = a1.at[pl.ds(HALF, HALF), src, :, pl.ds(128 * j, 128)]
                copy(half, half, ag1_ls.at[1], ag1_r.at[j, s], {"batch_1": xl}).start()

    def far_step(s):
        src = (z + NZ - slot_shift(s)) % NZ
        for j in range(2):
            r = (x + NX - first - j) % NX

            @pl.when(r == 2)
            def _():
                arrived(a1.at[pl.ds(0, FIELDS), src, :, pl.ds(128 * j, 128)], ag1_r.at[j, s])

    def owned(who, src, act):
        whole = src // 4 == who % 2

        @pl.when(whole)
        def _():
            act(HALF * (who // 2) + 6 * (who % 2), 7)

        @pl.when(jnp.logical_not(whole))
        def _():
            act(HALF * (who // 2) + 7 * (who % 2), 6)

    def second_send(s):
        src = (z + NZ - slot_shift(s)) % NZ

        def act(field, n):
            mineh = cur1.at[pl.ds(field - base, n), src]
            there = a2.at[pl.ds(field, n), src]
            copy(mineh, there, ag2_s.at[0], ag2_r.at[s, 0], {"batch_1": xr}).start()
            copy(mineh, there, ag2_s.at[1], ag2_r.at[s, 1], {"batch_1": xl}).start()
            there[...] = mineh[...]

        owned(x, src, act)

    def second_step(s):
        src = (z + NZ - slot_shift(s)) % NZ
        for d, who, to in ((0, xl, xr), (1, xr, xl)):
            def act(field, n):
                piece = a2.at[pl.ds(field, n), src]
                arrived(piece, ag2_r.at[s, d])

                @pl.when(src % 2 == 1 - d)
                def _():
                    copy(piece, piece, ag2_ls.at[d], ag2_lr.at[s], {"batch_1": to}).start()

            owned(who, src, act)

    def second_far(s):
        src = (z + NZ - slot_shift(s)) % NZ

        def act(field, n):
            arrived(a2.at[pl.ds(field, n), src], ag2_lr.at[s])

        owned((x + 2) % NX, src, act)

    def crossed(to):
        def act(field, n):
            for j in range(2):
                copy(
                    cur2.at[pl.ds(field - base, n), to, :, lanes(j)],
                    out.at[pl.ds(field - HALF * wide, n), :, lanes(z)],
                    o_s, o_r, {"batch_1": first + j, "dim": to, "field": wide},
                ).start()

        owned(x, to, act)

    def layer(level, group):
        srcs = [(z + NZ - slot_shift(GROUP * group + g)) % NZ for g in range(GROUP)]
        rows = BLK * SUB

        def stacked(ref):
            return jnp.concatenate([ref(src).reshape(rows, -1) for src in srcs], axis=0)

        rhs = (a2 if level else a1)[...].reshape(KW, 256)
        prod = jnp.dot(stacked(lambda src: w[level, :, src]), rhs, preferred_element_type=F32)
        for g, src in enumerate(srcs):
            anchor = a1[pl.ds(base, BLK), src].reshape(rows, 256).astype(F32)
            before = cur1[:, src].reshape(rows, 256).astype(F32) if level else anchor
            nxt = (anchor * prod[g * rows : (g + 1) * rows] + before).astype(BF16).reshape(BLK, SUB, 256)
            if level:
                cur2[:, src] = nxt
            else:
                cur1[:, src] = nxt

        for g, src in enumerate(srcs):
            if level:
                crossed(src)
            else:
                second_send(GROUP * group + g)

    def rows_here(level, s):
        src = (z + NZ - slot_shift(s)) % NZ

        @pl.when(c == wide)
        def _():
            arrived(w.at[level, :, src, :, pl.ds(0, 3 * KA)], dy_r.at[level, s])

    def each(low, high, step):
        @pl.loop(low, high)
        def _(s):
            step(s)

    def at(i, plan, step):
        for due, low, high in plan:
            @pl.when(i == due)
            def _():
                each(low, high, step)

    def layers(level, low, high):
        @pl.loop(low // GROUP, high // GROUP)
        def _(k):
            for g in range(GROUP):
                rows_here(level, GROUP * k + g)
            layer(level, k)

    @pl.when(c == wide)
    def _():
        from_a(0, 0)
        copy(
            feat.at[:, :, lanes(z)],
            a1.at[pl.ds(HALF * c, HALF), z, :, lanes(p)],
            a2a_s.at[1], a2a_r.at[0], {"field": tall},
        ).start()
        hand_over(1, 0)
        examples_out(1, 3)

        @pl.loop(1, 13)
        def _(i):
            @pl.when(i < NZ)
            def _():
                from_a(0, i)

            for due, low, high in ((2, 3, 5), (4, 5, 7), (5, 7, 8)):
                @pl.when(i == due)
                def _():
                    examples_out(low, high)

            @pl.when((i >= 2) & (i < 10))
            def _():
                from_b(0, i - 2)

            @pl.when(i >= 6)
            def _():
                from_a(1, i - 6)

            at(i, ((5, 0, 1), (6, 1, 2), (7, 2, 3), (8, 3, 4), (9, 4, 6), (10, 6, 8)), relay_step)

            @pl.when(i == 8)
            def _():
                tower_step(0)

            @pl.when(i == 11)
            def _():
                from_b(1, 0)
                tower_step(1)
                tower_step(2)
                each(0, NZ, far_step)
                layers(0, 0, 4)

        layers(0, 4, NZ)
        each(1, 3, functools.partial(from_b, 1))
        from_a(1, 7)

    @pl.when(c == tall)
    def _():
        examples_out(1, 3)
        to_y(0, 0)
        to_y(1, 0)
        for step in range(1, NX):
            to = (x + step) % NX
            copy(
                c_own, cands.at[NX * y + x], c_s.at[0], c_r.at[0], {"batch_1": to, "field": 1 - to // 2}
            ).start()
        example_step(0)
        from_y(0, 0)

        @pl.loop(1, 11)
        def _(i):
            @pl.when(i < NZ)
            def _():
                to_y(0, i)

            for due in (1, 2, 3):
                @pl.when(i == due)
                def _():
                    examples_out(2 * due + 1, min(2 * due + 3, NZ))

            @pl.when(i == 1)
            def _():
                from_y(1, 0)

            @pl.when((i > 1) & (i < NZ + 1))
            def _():
                from_y(0, i - 1)

            at(i, ((2, 1, 2), (3, 2, 3), (4, 3, 5), (5, 5, 7), (6, 7, 8)), example_step)

            @pl.when(i >= 8)
            def _():
                to_y(1, i - 7)

            @pl.when(i >= 3)
            def _():
                to_core(0, i - 3)

            at(i, ((3, 0, 1), (4, 1, 2), (5, 2, 3), (6, 3, 5), (7, 5, 7), (8, 7, 8)), relay_step)

            @pl.when(i == 4)
            def _():
                to_core(1, 0)

            @pl.when(i == 5)
            def _():
                tower_step(0)

            @pl.when(i == 9)
            def _():
                tower_step(1)
                tower_step(2)
                arrived(w.at[0, :, :, :, rest], db_r.at[0])
                layers(0, 0, 4)

        to_y(1, 4)
        layers(0, 4, NZ)

    @pl.when(c == wide)
    def _():
        each(0, 3, second_step)
        each(3, 5, functools.partial(from_b, 1))
        each(3, 5, tower_step)
        each(3, NZ, second_step)
        each(5, 7, functools.partial(from_b, 1))
        each(5, 7, tower_step)
        from_b(1, 7)

    @pl.when(c == tall)
    def _():
        @pl.loop(1, NZ)
        def _(i):
            from_y(1, i)

            @pl.when(i < 4)
            def _():
                to_y(1, i + 4)

            for due, low, high in ((2, 3, 5), (5, 5, 7), (7, 7, 8)):
                @pl.when(i == due)
                def _():
                    each(low, high, tower_step)

            @pl.when((i > 1) & (i < 6))
            def _():
                each(2 * i - 4, 2 * i - 2, second_step)

            @pl.when(i >= 4)
            def _():
                to_core(1, i - 3)

        to_core(1, 5)
        arrived(w.at[1, :, :, :, rest], db_r.at[1])

    @pl.loop(0, NZ)
    def _(s):
        second_far(s)

    layers(1, 0, 4)

    @pl.when(c == wide)
    def _():
        tower_step(7)

    @pl.when(c == tall)
    def _():
        to_core(1, 6)
        to_core(1, 7)
        got = cands.at[pl.ds(NX * y, NX)]
        arrived(cands.at[pl.ds(NX * y, NX - 1)], c_r.at[0])
        for step in range(1, NX):
            copy(got, got, c_s.at[1], c_r.at[1], {"batch_0": (y + step) % NX}).start()

    layers(1, 4, NZ)

    arrived(t.at[:, c], td_r)

    def tower(k):
        lhs = t[pl.ds(2 * k, 2), :, :, 0 : BLK * 128].reshape(256, BLK * 128)
        prod = jnp.dot(lhs, cur2[...].reshape(BLK * 128, 256), preferred_element_type=F32)
        part[pl.ds(256 * k, 256)] = prod.astype(BF16)
        mine[pl.ds(256 * k, 256)] = prod

    def far_sum(h):
        for j in range(2):
            @pl.when((x + NX - first - j) % NX == 2)
            def _():
                to = (xr, xl)[h]
                copy(
                    part.at[pl.ds(512 * h, 512), pl.ds(128 * j, 128)], hop, rs_s.at[h], hop_r, {"batch_1": to}
                ).start()

    for h in range(2):
        @pl.loop(2 * h, 2 * h + 2)
        def _(k):
            tower(k)

        far_sum(h)

    for r, own, added, way in ((1, 0, 512, xl), (3, 512, 0, xr)):
        for j in range(2):
            @pl.when((x + NX - first - j) % NX == r)
            def _():
                cols = pl.ds(128 * j, 128)
                slot = rs.at[r // 2]
                copy(
                    part.at[pl.ds(own, 512), cols], slot.at[pl.ds(own, 512)], rs_s.at[2], rs_r, {"batch_1": way}
                ).start()
                arrived(hop, hop_r)
                summed[...] = (mine[pl.ds(added, 512), cols] + hop[...].astype(F32)).astype(BF16)
                copy(summed, slot.at[pl.ds(added, 512)], rs_s.at[3], rs_r, {"batch_1": way}).start()

    @pl.when(c == tall)
    def _():
        arrived(rs, rs_r)

    for j in range(2):
        r = (x + NX - first - j) % NX

        @pl.when(r == 2)
        def _():
            arrived(hop, rs_s.at[0])
            arrived(hop, rs_s.at[1])

        @pl.when((r == 1) | (r == 3))
        def _():
            arrived(hop, rs_s.at[2])
            arrived(hop, rs_s.at[3])

    @pl.when(c == tall)
    def _():
        here = lanes(p)
        bias = t[:, :, :, BLK * 128 + 128 :].reshape(UNITS, 128).astype(F32)
        bias = bias[:, 0:1] + bias[:, 1:2] + bias[:, 2:3]
        total = mine[:, here] + rs[0].astype(F32) + rs[1].astype(F32)
        hidden = jnp.maximum(total + bias, 0.0).astype(BF16)
        qw = t[:, :, :, BLK * 128 : BLK * 128 + 128].reshape(UNITS, 128)
        query = lax.dot_general(qw, hidden, (((0,), (0,)), ((), ())), preferred_element_type=F32)
        u_copy.wait()
        query = (query + u_own[...].astype(F32).T).astype(BF16)

        arrived(cands.at[pl.ds(0, 3 * NX)], c_r.at[1])
        scale = 1.0 / math.sqrt(128)

        def scores(k, top):
            got = jnp.dot(cands[k], query, preferred_element_type=F32) * scale
            logits[k] = got
            return jnp.maximum(top, jnp.max(got.reshape(32, 8, 128), axis=0))

        top = lax.fori_loop(0, NX * NX, scores, jnp.full((8, 128), -1e30, F32), unroll=4)
        top = jnp.max(top, axis=0, keepdims=True)
        wanted = target[pl.ds(z, 1), :]
        index = lax.broadcasted_iota(jnp.int32, (256, 128), 0)

        def fold(k, carry):
            total, picked = carry
            got = logits[k]
            e = jnp.exp(got - top)
            hit = jnp.where(index == wanted - 256 * k, got, 0.0)
            return (
                total + jnp.sum(e.reshape(32, 8, 128), axis=0),
                picked + jnp.sum(hit.reshape(32, 8, 128), axis=0),
            )

        zero = jnp.zeros((8, 128), F32)
        total, picked = lax.fori_loop(0, NX * NX, fold, (zero, zero), unroll=4)
        total = jnp.sum(total, axis=0, keepdims=True)
        picked = jnp.sum(picked, axis=0, keepdims=True)
        result = top + jnp.log(total) - picked
        loss[z] = jnp.broadcast_to(result, (8, 128))

        @pl.loop(1, NZ)
        def _(dz):
            to = (z + dz) % NZ
            copy(loss.at[z], loss.at[z], g_s.at[0], g_r, {"dim": to}).start()
            copy(loss.at[z], loss.at[z], g_s.at[1], g_r, {"dim": to, "field": wide}).start()

        copy(loss.at[z], loss.at[z], g_s.at[2], g_r, {"field": wide}).start()
        arrived(loss.at[pl.ds(0, NZ - 1)], g_r)
        arrived(loss.at[pl.ds(0, NZ - 1)], g_s.at[0])
        arrived(loss.at[pl.ds(0, NZ - 1)], g_s.at[1])
        arrived(loss.at[0], g_s.at[2])
        arrived(cands.at[pl.ds(0, 3)], c_s.at[0])
        arrived(cands.at[pl.ds(0, 3 * NX)], c_s.at[1])
        for d in range(2):
            arrived(a1.at[pl.ds(0, FIELDS), :, :, pl.ds(0, 128)], ag1_s.at[d])
        for level in range(2):
            for d in range(2):
                arrived(w.at[level, :, :, :, pl.ds(0, KA)], y_s.at[level, d])
            arrived(w.at[level, pl.ds(0, 4), :, :, pl.ds(0, KA)], l_s.at[level, 0])
            arrived(w.at[level, pl.ds(4, 3), :, :, pl.ds(0, KA)], l_s.at[level, 1])
            arrived(w.at[level, :, :, :, pl.ds(0, 3 * KA)], dy_s.at[level])

    @pl.when(c == wide)
    def _():
        arrived(loss, g_r)
        arrived(feat.at[:, :, pl.ds(0, 128)], a2a_s.at[1])
        for level in range(2):
            arrived(w.at[level, :, pl.ds(0, 4), :, pl.ds(0, KA)], z_s.at[level, 0, 0])
            arrived(w.at[level, :, pl.ds(0, 3), :, pl.ds(0, KA)], z_s.at[level, 1, 0])
            arrived(w.at[level, :, pl.ds(0, 3), :, rest], z_s.at[level, 0, 1])
            arrived(w.at[level, :, pl.ds(0, 4), :, rest], z_s.at[level, 1, 1])
            arrived(w.at[level, :, :, :, pl.ds(0, KA)], da_s.at[level])
            arrived(w.at[level, :, :, :, rest], db_s.at[level])

    arrived(feat.at[:, :, pl.ds(0, 128 * (NZ - 1))], a2a_s.at[0])
    for j in range(2):
        r = (x + NX - first - j) % NX

        @pl.when(r == 1)
        def _():
            arrived(a1.at[pl.ds(0, HALF), :, :, pl.ds(0, 128)], ag1_ls.at[0])

        @pl.when(r == 3)
        def _():
            arrived(a1.at[pl.ds(0, HALF), :, :, pl.ds(0, 128)], ag1_ls.at[1])

    for d in range(2):
        arrived(a2.at[pl.ds(0, HALF), pl.ds(0, 4)], ag2_s.at[d])
        arrived(a2.at[pl.ds(0, HALF), pl.ds(0, 2)], ag2_ls.at[d])
    for d in range(2):
        arrived(t.at[pl.ds(0, 3), 0], t_s.at[d])
        arrived(t.at[0, 0, pl.ds(0, 32)], t_s.at[2 + d])
    arrived(t.at[:, 0], td_s)
    arrived(a1.at[pl.ds(0, HALF), :, :, pl.ds(0, 128)], o_s)
    for k in range(NZ):
        loss_out[k : k + 1] = loss[k, 0:1]
    arrived(out, o_r)


def body(features, cross_weight, cross_bias, tower_weight, tower_bias, query_weight, user_vec, candidates, positive):
    vmem = pl.BlockSpec(memory_space=pltpu.VMEM)
    hbm = pl.BlockSpec(memory_space=pl.ANY)
    dma = pltpu.SemaphoreType.DMA
    out, loss = pl.pallas_call(
        kernel,
        out_shape=(
            pltpu.VMEM((HALF, SUB, 1024), BF16),
            pltpu.VMEM((NZ, 128), F32),
        ),
        in_specs=[vmem, hbm, vmem, hbm, vmem, vmem, vmem, hbm, vmem],
        out_specs=(vmem, vmem),
        scratch_shapes=[
            pltpu.VMEM((KB, NZ, SUB, 256), BF16),
            pltpu.VMEM((KB, NZ, SUB, 256), BF16),
            pltpu.VMEM((2, BLK, NZ, SUB, KW), BF16),
            pltpu.VMEM((NZ, 2, 64, TC), BF16),
            pltpu.VMEM((BLK, NZ, SUB, 256), BF16),
            pltpu.VMEM((BLK, NZ, SUB, 256), BF16),
            pltpu.VMEM((UNITS, 256), BF16),
            pltpu.VMEM((UNITS, 256), F32),
            pltpu.VMEM((2, UNITS, 128), BF16),
            pltpu.VMEM((UNITS // 2, 128), BF16),
            pltpu.VMEM((UNITS // 2, 128), BF16),
            pltpu.VMEM((NX * NX, 256, 128), BF16),
            pltpu.VMEM((NX * NX, 256, 128), F32),
            pltpu.VMEM((128, 128), BF16),
            pltpu.VMEM((NZ, 8, 128), F32),
            dma((2,)), dma, dma,
            dma((2,)), dma((NZ,)),
            dma((2,)), dma((2, NZ)), dma((2,)),
            dma((2,)), dma((NZ, 2)), dma((2,)), dma((NZ,)),
            dma((2, 2, 2)), dma((2, NZ, 2)),
            dma((2, 2)), dma((2, NZ, 2)),
            dma((2, 2)), dma((2, NZ)),
            dma((2,)), dma((2, NZ)), dma((2,)), dma((2,)), dma((2,)), dma((2, NZ)),
            dma((4,)), dma((9,)), dma, dma,
            dma((2,)), dma((2,)),
            dma((4,)), dma, dma,
            dma, dma,
            dma((3,)), dma,
        ],
        compiler_params=pltpu.CompilerParams(collective_id=0, has_side_effects=True, vmem_limit_bytes=60 * 1024 * 1024),
        name="dcn",
    )(
        features,
        cross_weight.transpose(0, 1, 3, 2, 4),
        cross_bias.transpose(1, 0, 2),
        tower_weight.transpose(1, 0, 2),
        tower_bias.reshape(1, 64),
        query_weight,
        candidates,
        user_vec,
        positive.reshape(NZ, 128),
    )
    return out, loss.reshape(1024)


def solution(mesh):
    torus = Mesh(
        mesh.devices.reshape(4, 4, mesh.shape["field"], mesh.shape["dim"]),
        ("batch_0", "batch_1", "field", "dim"),
    )
    in_specs = (
        P("field", "dim", BATCH),
        P(None, "field", "dim", None, None),
        P(None, "field", "dim"),
        P(("field", "dim"), None, None),
        P(("field", "dim")),
        P(("field", "dim"), None),
        P(BATCH, None),
        P(BATCH, None),
        P(BATCH),
    )
    out_specs = (P("field", "dim", BATCH), P(BATCH))
    return jax.shard_map(body, mesh=torus, in_specs=in_specs, out_specs=out_specs, check_vma=False)
```

```python
import functools
import math

import jax
import jax.numpy as jnp
from jax import lax
from jax.experimental import pallas as pl
from jax.experimental.pallas import tpu as pltpu
from jax.sharding import Mesh
from jax.sharding import PartitionSpec as P

BATCH = ("batch_0", "batch_1")
MESH = pl.DeviceIdType.MESH
F32 = jnp.float32
BF16 = jnp.bfloat16

FIELDS = 26
NX = 4
NZ = 8
HALF = 13
SUB = 16
BLK = 7
NY = 6
NREST = FIELDS + 1 - NX * NY
KB = FIELDS + 1
KA = NY * 128
KR = NREST * 128
KW = KB * 128
GROUP = 2
TC = BLK * 128 + 256
UNITS = 1024


def copy(src, dst, send, recv, where):
    return pltpu.make_async_remote_copy(
        src_ref=src, dst_ref=dst, send_sem=send, recv_sem=recv, device_id=where, device_id_type=MESH
    )


def arrived(ref, sem):
    pltpu.make_async_copy(ref, ref, sem).wait()


def slot_shift(s):
    return jnp.where(s % 2 == 1, (s + 1) // 2, (NZ - s // 2) % NZ)


def kernel(
    feat, c_w, c_b, t_w, t_b, q_w, c_own, user, target,
    out, loss_out,
    a1, a2, w, t, cur1, cur2, part, mine, rs, hop, summed, cands, logits, u_own, loss,
    w_l, t_l, u_l,
    a2a_s, a2a_r, ag1_s, ag1_r, ag1_ls, ag2_s, ag2_r, ag2_ls, ag2_lr,
    z_s, z_r, y_s, y_r, l_s, l_r, da_s, da_r, db_s, db_r, dy_s, dy_r,
    t_s, t_r, td_s, td_r, c_s, c_r, rs_s, rs_r, hop_r, o_s, o_r, g_s, g_r,
):
    x = lax.axis_index("batch_1")
    y = lax.axis_index("batch_0")
    z = lax.axis_index("dim")
    c = lax.axis_index("field")
    p = x % 2
    wide = x // 2
    tall = 1 - wide
    xr, xl = (x + 1) % NX, (x + NX - 1) % NX
    yr, yl = (y + 1) % NX, (y + NX - 1) % NX
    zr, zl = (z + 1) % NZ, (z + NZ - 1) % NZ
    first = 2 * (1 - c)

    def lanes(j):
        return pl.ds(pl.multiple_of(j * 128, 128), 128)

    def ycols(who):
        return pl.ds(pl.multiple_of(who * KA, 128), KA)

    rest = pl.ds(NX * NY * 128, KR)

    barrier = pltpu.get_barrier_semaphore()

    def greet(where):
        pl.semaphore_signal(barrier, inc=1, device_id=where, device_id_type=MESH)

    for step in range(1, NX):
        for core in range(2):
            greet({"batch_1": (x + step) % NX, "field": core})
        greet({"batch_0": (y + step) % NX})
    for step in range(1, NZ):
        for core in range(2):
            greet({"dim": (z + step) % NZ, "field": core})
    greet({"field": 1 - c})

    base = HALF * wide + 6 * p
    own_w = [(level, k) for level in range(2) for k in range(NY + NREST - 1)]

    def own_copy(level, k):
        field = NY * y + k if k < NY else NX * NY + k - NY
        return pltpu.make_async_copy(
            c_w.at[level, pl.ds(6 * p, BLK), field], w.at[level, :, z, :, lanes(field)], w_l.at[level]
        )

    @pl.when(c == wide)
    def _():
        for level, k in own_w:
            own_copy(level, k).start()

    t_copies = [
        pltpu.make_async_copy(t_w.at[base + k], t.at[z, c, :, pl.ds(128 * k, 128)], t_l)
        for k in range(BLK)
    ]
    for cp in t_copies:
        cp.start()

    u_copy = pltpu.make_async_copy(user.at[pl.ds(pl.multiple_of(128 * z, 128), 128)], u_own, u_l)

    @pl.when(c == tall)
    def _():
        u_copy.start()

    row = lax.broadcasted_iota(jnp.int32, (NZ, SUB, 256), 0) * SUB + lax.broadcasted_iota(
        jnp.int32, (NZ, SUB, 256), 1
    )
    ones = jnp.where(row < 3, 1.0, 0.0).astype(BF16)
    a1[FIELDS] = ones
    a2[FIELDS] = ones

    def bias_block(values):
        n = values.shape[1]
        eye = lax.broadcasted_iota(jnp.int32, (n, n), 0) == lax.broadcasted_iota(jnp.int32, (n, n), 1)
        col = jnp.sum(jnp.where(eye, values, 0.0), axis=1, keepdims=True)
        hi = col.astype(BF16).astype(F32)
        mid = (col - hi).astype(BF16).astype(F32)
        low = (col - hi) - mid
        lane = lax.broadcasted_iota(jnp.int32, (n, 128), 1)
        terms = jnp.where(lane == 0, hi, jnp.where(lane == 1, mid, jnp.where(lane == 2, low, 0.0)))
        return terms.astype(BF16)

    t[z, c, :, BLK * 128 : BLK * 128 + 128] = q_w[...]
    t[z, c, :, BLK * 128 + 128 :] = bias_block(t_b[...])

    @pl.when(c == wide)
    def _():
        @pl.loop(0, BLK)
        def _(f):
            for level in range(2):
                w[level, f, z, :, FIELDS * 128 :] = bias_block(c_b[6 * p + f, level : level + 1])

        for level in range(2):
            arrived(w.at[level, :, z, :, pl.ds(0, 128 * (NY + NREST - 1))], w_l.at[level])

    @pl.when(c == tall)
    def _():
        a1[pl.ds(HALF * c, HALF), z, :, lanes(p)] = feat[:, :, lanes(z)]
        cands[NX * y + x] = c_own[...]

    arrived(t.at[z, c, :, pl.ds(0, 128 * BLK)], t_l)
    lane64 = lax.broadcasted_iota(jnp.int32, (64, 128), 1)
    edge = lanes((BLK - 1) * (1 - p))
    kept = (lane64 < 64) == (p == 0)
    t[z, c, :, edge] = jnp.where(kept, t[z, c, :, edge].astype(F32), 0.0).astype(BF16)

    pl.semaphore_wait(barrier, 3 * NX - 3 + 2 * NZ - 2 + 1)

    def examples_out(low, high):
        @pl.loop(low, high)
        def _(s):
            to = (z + slot_shift(s)) % NZ
            copy(
                feat.at[:, :, lanes(to)],
                a1.at[pl.ds(HALF * c, HALF), z, :, lanes(p)],
                a2a_s.at[0], a2a_r.at[slot_shift(s)], {"dim": to, "field": tall},
            ).start()

    def along_z(ref, level, s, k, d):
        to = jnp.where(d == 0, zr, zl)
        nxt = jnp.where(s == 0, 1 + d, jnp.minimum(s + 2, NZ - 1))
        copy(ref, ref, z_s.at[level, d, k], z_r.at[level, nxt, k], {"dim": to}).start()

    def hand_over(level, s):
        ref = w.at[level, :, (z + NZ - slot_shift(s)) % NZ, :, ycols(y)]
        copy(ref, ref, da_s.at[level], da_r.at[level, s], {"field": 1 - c}).start()

    def from_z(level, s, k):
        src = (z + NZ - slot_shift(s)) % NZ
        ref = w.at[level, :, src, :, rest] if k else w.at[level, :, src, :, ycols(y)]
        onward = ((s < 5) | (s == 6)) if k else (s < 6)

        @pl.when(s > 0)
        def _():
            arrived(ref, z_r.at[level, s, k])

        @pl.when((s > 0) & onward)
        def _():
            along_z(ref, level, s, k, jnp.where(s % 2 == 1, 0, 1))

        @pl.when(s == 0)
        def _():
            along_z(ref, level, s, k, 0)
            along_z(ref, level, s, k, 1)

        if k:
            copy(ref, ref, db_s.at[level], db_r.at[level], {"field": 1 - c}).start()
        elif level == 0:
            hand_over(level, s)
        else:
            @pl.when(s > 0)
            def _():
                hand_over(level, s)

    def from_a(level, s):
        from_z(level, s, 0)

    def from_b(level, s):
        from_z(level, s, 1)

    def to_y(level, s):
        src = (z + NZ - slot_shift(s)) % NZ
        own = w.at[level, :, src, :, ycols(y)]
        arrived(own, da_r.at[level, s])
        copy(own, own, y_s.at[level, 0], y_r.at[level, s, 0], {"batch_0": yr}).start()
        copy(own, own, y_s.at[level, 1], y_r.at[level, s, 1], {"batch_0": yl}).start()

    def from_y(level, s):
        src = (z + NZ - slot_shift(s)) % NZ
        left = w.at[level, :, src, :, ycols(yl)]
        right = w.at[level, :, src, :, ycols(yr)]
        up = w.at[level, pl.ds(0, 4), src, :, ycols(yl)]
        down = w.at[level, pl.ds(4, 3), src, :, ycols(yr)]
        arrived(left, y_r.at[level, s, 0])
        copy(up, up, l_s.at[level, 0], l_r.at[level, s], {"batch_0": yr}).start()
        copy(left, left, dy_s.at[level], dy_r.at[level, s], {"field": 1 - c}).start()
        arrived(right, y_r.at[level, s, 1])
        copy(down, down, l_s.at[level, 1], l_r.at[level, s], {"batch_0": yl}).start()
        copy(right, right, dy_s.at[level], dy_r.at[level, s], {"field": 1 - c}).start()

    def to_core(level, s):
        src = (z + NZ - slot_shift(s)) % NZ
        far = (y + 2) % NX
        piece = w.at[level, :, src, :, ycols(far)]
        arrived(piece, l_r.at[level, s])
        copy(piece, piece, dy_s.at[level], dy_r.at[level, s], {"field": 1 - c}).start()

    def tower_step(s):
        src = (z + NZ - slot_shift(s)) % NZ
        whole = t.at[src, c]

        @pl.when(s == 0)
        def _():
            copy(whole, whole, t_s.at[0], t_r.at[1], {"dim": zr}).start()
            copy(whole, whole, t_s.at[1], t_r.at[2], {"dim": zl}).start()

        @pl.when((s > 0) & (s < 7))
        def _():
            arrived(whole, t_r.at[s])

        for par, to in ((1, zr), (0, zl)):
            d = 1 - par
            half = t.at[src, c, pl.ds(32 * d, 32)]

            @pl.when((s > 0) & (s < 5) & (s % 2 == par))
            def _():
                copy(whole, whole, t_s.at[d], t_r.at[s + 2], {"dim": to}).start()

            @pl.when(s == 6 - par)
            def _():
                copy(half, half, t_s.at[2 + d], t_r.at[7 + d], {"dim": to}).start()

        @pl.when(s == 7)
        def _():
            arrived(t.at[src, c, pl.ds(0, 32)], t_r.at[7])
            arrived(t.at[src, c, pl.ds(32, 32)], t_r.at[8])

        copy(whole, whole, td_s, td_r, {"field": 1 - c}).start()

    def example_step(s):
        dz = slot_shift(s)
        src = (z + NZ - dz) % NZ
        whole = a1.at[pl.ds(0, FIELDS), src, :, lanes(p)]

        @pl.when(s == 0)
        def _():
            arrived(a1.at[pl.ds(0, HALF), src, :, lanes(p)], a2a_r.at[0])

        @pl.when(s > 0)
        def _():
            arrived(whole, a2a_r.at[dz])

        copy(whole, whole, ag1_s.at[0], ag1_r.at[p, s], {"batch_1": xr}).start()
        copy(whole, whole, ag1_s.at[1], ag1_r.at[p, s], {"batch_1": xl}).start()

    def relay_step(s):
        src = (z + NZ - slot_shift(s)) % NZ
        for j in range(2):
            r = (x + NX - first - j) % NX
            whole = a1.at[pl.ds(0, FIELDS), src, :, pl.ds(128 * j, 128)]

            @pl.when(r == 1)
            def _():
                arrived(whole, ag1_r.at[j, s])
                half = a1.at[pl.ds(0, HALF), src, :, pl.ds(128 * j, 128)]
                copy(half, half, ag1_ls.at[0], ag1_r.at[j, s], {"batch_1": xr}).start()

            @pl.when(r == 3)
            def _():
                arrived(whole, ag1_r.at[j, s])
                half = a1.at[pl.ds(HALF, HALF), src, :, pl.ds(128 * j, 128)]
                copy(half, half, ag1_ls.at[1], ag1_r.at[j, s], {"batch_1": xl}).start()

    def far_step(s):
        src = (z + NZ - slot_shift(s)) % NZ
        for j in range(2):
            r = (x + NX - first - j) % NX

            @pl.when(r == 2)
            def _():
                arrived(a1.at[pl.ds(0, FIELDS), src, :, pl.ds(128 * j, 128)], ag1_r.at[j, s])

    def owned(who, src, act):
        whole = src // 4 == who % 2

        @pl.when(whole)
        def _():
            act(HALF * (who // 2) + 6 * (who % 2), 7)

        @pl.when(jnp.logical_not(whole))
        def _():
            act(HALF * (who // 2) + 7 * (who % 2), 6)

    def second_send(s):
        src = (z + NZ - slot_shift(s)) % NZ

        def act(field, n):
            mineh = cur1.at[pl.ds(field - base, n), src]
            there = a2.at[pl.ds(field, n), src]
            copy(mineh, there, ag2_s.at[0], ag2_r.at[s, 0], {"batch_1": xr}).start()
            copy(mineh, there, ag2_s.at[1], ag2_r.at[s, 1], {"batch_1": xl}).start()
            there[...] = mineh[...]

        owned(x, src, act)

    def second_step(s):
        src = (z + NZ - slot_shift(s)) % NZ
        for d, who, to in ((0, xl, xr), (1, xr, xl)):
            def act(field, n):
                piece = a2.at[pl.ds(field, n), src]
                arrived(piece, ag2_r.at[s, d])

                @pl.when(src % 2 == 1 - d)
                def _():
                    copy(piece, piece, ag2_ls.at[d], ag2_lr.at[s], {"batch_1": to}).start()

            owned(who, src, act)

    def second_far(s):
        src = (z + NZ - slot_shift(s)) % NZ

        def act(field, n):
            arrived(a2.at[pl.ds(field, n), src], ag2_lr.at[s])

        owned((x + 2) % NX, src, act)

    def crossed(to, j):
        def act(field, n):
            copy(
                cur2.at[pl.ds(field - base, n), to, :, lanes(j)],
                out.at[pl.ds(field - HALF * wide, n), :, lanes(z)],
                o_s, o_r, {"batch_1": first + j, "dim": to, "field": wide},
            ).start()

        owned(x, to, act)

    def crossed_away(to):
        @pl.when(c == wide)
        def _():
            crossed(to, 0)
            crossed(to, 1)

        @pl.when(c == tall)
        def _():
            crossed(to, 1 - p)

    def layer(level, group):
        srcs = [(z + NZ - slot_shift(GROUP * group + g)) % NZ for g in range(GROUP)]
        rows = BLK * SUB

        def stacked(ref):
            return jnp.concatenate([ref(src).reshape(rows, -1) for src in srcs], axis=0)

        rhs = (a2 if level else a1)[...].reshape(KW, 256)
        prod = jnp.dot(stacked(lambda src: w[level, :, src]), rhs, preferred_element_type=F32)
        for g, src in enumerate(srcs):
            anchor = a1[pl.ds(base, BLK), src].reshape(rows, 256).astype(F32)
            before = cur1[:, src].reshape(rows, 256).astype(F32) if level else anchor
            nxt = (anchor * prod[g * rows : (g + 1) * rows] + before).astype(BF16).reshape(BLK, SUB, 256)
            if level:
                cur2[:, src] = nxt
            else:
                cur1[:, src] = nxt

        for g, src in enumerate(srcs):
            if level:
                @pl.when(c == tall)
                def _():
                    crossed(src, p)

                @pl.when(GROUP * group < 4)
                def _():
                    crossed_away(src)
            else:
                second_send(GROUP * group + g)

    def rows_here(level, s):
        src = (z + NZ - slot_shift(s)) % NZ

        @pl.when(c == wide)
        def _():
            arrived(w.at[level, :, src, :, pl.ds(0, 3 * KA)], dy_r.at[level, s])

    def each(low, high, step):
        @pl.loop(low, high)
        def _(s):
            step(s)

    def at(i, plan, step):
        for due, low, high in plan:
            @pl.when(i == due)
            def _():
                each(low, high, step)

    def layers(level, low, high):
        @pl.loop(low // GROUP, high // GROUP)
        def _(k):
            for g in range(GROUP):
                rows_here(level, GROUP * k + g)
            layer(level, k)

    @pl.when(c == wide)
    def _():
        from_a(0, 0)
        copy(
            feat.at[:, :, lanes(z)],
            a1.at[pl.ds(HALF * c, HALF), z, :, lanes(p)],
            a2a_s.at[1], a2a_r.at[0], {"field": tall},
        ).start()
        hand_over(1, 0)
        examples_out(1, 3)

        @pl.loop(1, 13)
        def _(i):
            @pl.when(i < NZ)
            def _():
                from_a(0, i)

            for due, low, high in ((2, 3, 5), (4, 5, 7), (5, 7, 8)):
                @pl.when(i == due)
                def _():
                    examples_out(low, high)

            @pl.when((i >= 2) & (i < 10))
            def _():
                from_b(0, i - 2)

            @pl.when(i >= 6)
            def _():
                from_a(1, i - 6)

            at(i, ((5, 0, 1), (6, 1, 2), (7, 2, 4), (8, 4, 7), (9, 7, 8)), relay_step)

            @pl.when(i == 8)
            def _():
                tower_step(0)

            @pl.when(i == 7)
            def _():
                from_b(1, 0)

            @pl.when(i == 11)
            def _():
                tower_step(1)
                tower_step(2)

            @pl.when(i == 10)
            def _():
                each(1, 3, functools.partial(from_b, 1))
                each(0, NZ, far_step)
                layers(0, 0, 4)

        layers(0, 4, NZ)
        each(3, 5, functools.partial(from_b, 1))
        from_a(1, 7)

    @pl.when(c == tall)
    def _():
        examples_out(1, 3)
        to_y(0, 0)
        to_y(1, 0)
        for step in range(1, NX):
            to = (x + step) % NX
            copy(
                c_own, cands.at[NX * y + x], c_s.at[0], c_r.at[0], {"batch_1": to, "field": 1 - to // 2}
            ).start()
        example_step(0)
        from_y(0, 0)

        @pl.loop(1, 11)
        def _(i):
            @pl.when(i < NZ)
            def _():
                to_y(0, i)

            for due in (1, 2, 3):
                @pl.when(i == due)
                def _():
                    examples_out(2 * due + 1, min(2 * due + 3, NZ))

            @pl.when(i == 1)
            def _():
                from_y(1, 0)

            @pl.when((i > 1) & (i < NZ + 1))
            def _():
                from_y(0, i - 1)

            at(i, ((2, 1, 2), (3, 2, 3), (4, 3, 5), (5, 5, 7), (6, 7, 8)), example_step)

            @pl.when(i >= 8)
            def _():
                to_y(1, i - 7)

            @pl.when(i >= 3)
            def _():
                to_core(0, i - 3)

            at(i, ((3, 0, 1), (4, 1, 2), (5, 2, 3), (6, 3, 5), (7, 5, 7), (8, 7, 8)), relay_step)

            @pl.when(i == 4)
            def _():
                to_core(1, 0)

            @pl.when(i == 5)
            def _():
                tower_step(0)

            @pl.when(i == 9)
            def _():
                tower_step(1)
                tower_step(2)
                arrived(w.at[0, :, :, :, rest], db_r.at[0])
                layers(0, 0, 4)

        to_y(1, 4)
        layers(0, 4, NZ)

    @pl.when(c == wide)
    def _():
        each(0, 2, second_step)
        each(3, 5, tower_step)
        each(2, NZ, second_step)
        each(5, 7, functools.partial(from_b, 1))
        each(5, 7, tower_step)
        from_b(1, 7)

    @pl.when(c == tall)
    def _():
        @pl.loop(1, NZ)
        def _(i):
            from_y(1, i)

            @pl.when(i < 4)
            def _():
                to_y(1, i + 4)

            for due, low, high in ((2, 3, 5), (5, 5, 7), (7, 7, 8)):
                @pl.when(i == due)
                def _():
                    each(low, high, tower_step)

            @pl.when((i > 1) & (i < 6))
            def _():
                each(2 * i - 4, 2 * i - 2, second_step)

            @pl.when(i >= 4)
            def _():
                to_core(1, i - 3)

        to_core(1, 5)
        arrived(w.at[1, :, :, :, rest], db_r.at[1])

    @pl.loop(0, NZ)
    def _(s):
        second_far(s)

    layers(1, 0, 4)

    @pl.when(c == wide)
    def _():
        tower_step(7)

    @pl.when(c == tall)
    def _():
        to_core(1, 6)
        to_core(1, 7)
        got = cands.at[pl.ds(NX * y, NX)]
        arrived(cands.at[pl.ds(NX * y, NX - 1)], c_r.at[0])
        for step in range(1, NX):
            copy(got, got, c_s.at[1], c_r.at[1], {"batch_0": (y + step) % NX}).start()

    layers(1, 4, NZ)

    arrived(t.at[:, c], td_r)

    def tower(k):
        lhs = t[pl.ds(2 * k, 2), :, :, 0 : BLK * 128].reshape(256, BLK * 128)
        prod = jnp.dot(lhs, cur2[...].reshape(BLK * 128, 256), preferred_element_type=F32)
        part[pl.ds(256 * k, 256)] = prod.astype(BF16)
        mine[pl.ds(256 * k, 256)] = prod

    def far_sum(k):
        for j in range(2):
            @pl.when((x + NX - first - j) % NX == 2)
            def _():
                copy(
                    part.at[pl.ds(256 * k, 256), pl.ds(128 * j, 128)],
                    hop.at[pl.ds(256 * (k % 2), 256)],
                    rs_s.at[k // 2], hop_r.at[k % 2], {"batch_1": (xr, xl)[k // 2]},
                ).start()

    for k in range(4):
        tower(k)
        far_sum(k)

    for r, own, added, way in ((1, 0, 512, xl), (3, 512, 0, xr)):
        for j in range(2):
            @pl.when((x + NX - first - j) % NX == r)
            def _():
                cols = pl.ds(128 * j, 128)
                slot = rs.at[r // 2]
                copy(
                    part.at[pl.ds(own, 512), cols], slot.at[pl.ds(own, 512)], rs_s.at[2], rs_r, {"batch_1": way}
                ).start()
                for q in range(2):
                    here, there = pl.ds(256 * q, 256), pl.ds(added + 256 * q, 256)
                    arrived(hop.at[here], hop_r.at[q])
                    summed[here] = (mine[there, cols] + hop[here].astype(F32)).astype(BF16)
                    copy(summed.at[here], slot.at[there], rs_s.at[3], rs_r, {"batch_1": way}).start()

    each(4, NZ, lambda s: crossed_away((z + NZ - slot_shift(s)) % NZ))

    @pl.when(c == tall)
    def _():
        arrived(rs, rs_r)

    for j in range(2):
        r = (x + NX - first - j) % NX

        @pl.when(r == 2)
        def _():
            arrived(hop, rs_s.at[0])
            arrived(hop, rs_s.at[1])

        @pl.when((r == 1) | (r == 3))
        def _():
            arrived(hop, rs_s.at[2])
            arrived(hop, rs_s.at[3])

    @pl.when(c == tall)
    def _():
        here = lanes(p)
        bias = t[:, :, :, BLK * 128 + 128 :].reshape(UNITS, 128).astype(F32)
        bias = bias[:, 0:1] + bias[:, 1:2] + bias[:, 2:3]
        total = mine[:, here] + rs[0].astype(F32) + rs[1].astype(F32)
        hidden = jnp.maximum(total + bias, 0.0).astype(BF16)
        qw = t[:, :, :, BLK * 128 : BLK * 128 + 128].reshape(UNITS, 128)
        query = lax.dot_general(qw, hidden, (((0,), (0,)), ((), ())), preferred_element_type=F32)
        u_copy.wait()
        query = (query + u_own[...].astype(F32).T).astype(BF16)

        arrived(cands.at[pl.ds(0, 3 * NX)], c_r.at[1])
        scale = 1.0 / math.sqrt(128)

        def scores(k, top):
            got = jnp.dot(cands[k], query, preferred_element_type=F32) * scale
            logits[k] = got
            return jnp.maximum(top, jnp.max(got.reshape(32, 8, 128), axis=0))

        top = lax.fori_loop(0, NX * NX, scores, jnp.full((8, 128), -1e30, F32), unroll=4)
        top = jnp.max(top, axis=0, keepdims=True)
        wanted = target[pl.ds(z, 1), :]
        index = lax.broadcasted_iota(jnp.int32, (256, 128), 0)

        def fold(k, carry):
            total, picked = carry
            got = logits[k]
            e = jnp.exp(got - top)
            hit = jnp.where(index == wanted - 256 * k, got, 0.0)
            return (
                total + jnp.sum(e.reshape(32, 8, 128), axis=0),
                picked + jnp.sum(hit.reshape(32, 8, 128), axis=0),
            )

        zero = jnp.zeros((8, 128), F32)
        total, picked = lax.fori_loop(0, NX * NX, fold, (zero, zero), unroll=4)
        total = jnp.sum(total, axis=0, keepdims=True)
        picked = jnp.sum(picked, axis=0, keepdims=True)
        result = top + jnp.log(total) - picked
        loss[z] = jnp.broadcast_to(result, (8, 128))

        @pl.loop(1, NZ)
        def _(dz):
            to = (z + dz) % NZ
            copy(loss.at[z], loss.at[z], g_s.at[0], g_r, {"dim": to}).start()
            copy(loss.at[z], loss.at[z], g_s.at[1], g_r, {"dim": to, "field": wide}).start()

        copy(loss.at[z], loss.at[z], g_s.at[2], g_r, {"field": wide}).start()
        arrived(loss.at[pl.ds(0, NZ - 1)], g_r)
        arrived(loss.at[pl.ds(0, NZ - 1)], g_s.at[0])
        arrived(loss.at[pl.ds(0, NZ - 1)], g_s.at[1])
        arrived(loss.at[0], g_s.at[2])
        arrived(cands.at[pl.ds(0, 3)], c_s.at[0])
        arrived(cands.at[pl.ds(0, 3 * NX)], c_s.at[1])
        for d in range(2):
            arrived(a1.at[pl.ds(0, FIELDS), :, :, pl.ds(0, 128)], ag1_s.at[d])
        for level in range(2):
            for d in range(2):
                arrived(w.at[level, :, :, :, pl.ds(0, KA)], y_s.at[level, d])
            arrived(w.at[level, pl.ds(0, 4), :, :, pl.ds(0, KA)], l_s.at[level, 0])
            arrived(w.at[level, pl.ds(4, 3), :, :, pl.ds(0, KA)], l_s.at[level, 1])
            arrived(w.at[level, :, :, :, pl.ds(0, 3 * KA)], dy_s.at[level])

    @pl.when(c == wide)
    def _():
        arrived(loss, g_r)
        arrived(feat.at[:, :, pl.ds(0, 128)], a2a_s.at[1])
        for level in range(2):
            arrived(w.at[level, :, pl.ds(0, 4), :, pl.ds(0, KA)], z_s.at[level, 0, 0])
            arrived(w.at[level, :, pl.ds(0, 3), :, pl.ds(0, KA)], z_s.at[level, 1, 0])
            arrived(w.at[level, :, pl.ds(0, 3), :, rest], z_s.at[level, 0, 1])
            arrived(w.at[level, :, pl.ds(0, 4), :, rest], z_s.at[level, 1, 1])
            arrived(w.at[level, :, :, :, pl.ds(0, KA)], da_s.at[level])
            arrived(w.at[level, :, :, :, rest], db_s.at[level])

    arrived(feat.at[:, :, pl.ds(0, 128 * (NZ - 1))], a2a_s.at[0])
    for j in range(2):
        r = (x + NX - first - j) % NX

        @pl.when(r == 1)
        def _():
            arrived(a1.at[pl.ds(0, HALF), :, :, pl.ds(0, 128)], ag1_ls.at[0])

        @pl.when(r == 3)
        def _():
            arrived(a1.at[pl.ds(0, HALF), :, :, pl.ds(0, 128)], ag1_ls.at[1])

    for d in range(2):
        arrived(a2.at[pl.ds(0, HALF), pl.ds(0, 4)], ag2_s.at[d])
        arrived(a2.at[pl.ds(0, HALF), pl.ds(0, 2)], ag2_ls.at[d])
    for d in range(2):
        arrived(t.at[pl.ds(0, 3), 0], t_s.at[d])
        arrived(t.at[0, 0, pl.ds(0, 32)], t_s.at[2 + d])
    arrived(t.at[:, 0], td_s)
    arrived(a1.at[pl.ds(0, HALF), :, :, pl.ds(0, 128)], o_s)
    for k in range(NZ):
        loss_out[k : k + 1] = loss[k, 0:1]
    arrived(out, o_r)


def body(features, cross_weight, cross_bias, tower_weight, tower_bias, query_weight, user_vec, candidates, positive):
    vmem = pl.BlockSpec(memory_space=pltpu.VMEM)
    hbm = pl.BlockSpec(memory_space=pl.ANY)
    dma = pltpu.SemaphoreType.DMA
    out, loss = pl.pallas_call(
        kernel,
        out_shape=(
            pltpu.VMEM((HALF, SUB, 1024), BF16),
            pltpu.VMEM((NZ, 128), F32),
        ),
        in_specs=[vmem, hbm, vmem, hbm, vmem, vmem, vmem, hbm, vmem],
        out_specs=(vmem, vmem),
        scratch_shapes=[
            pltpu.VMEM((KB, NZ, SUB, 256), BF16),
            pltpu.VMEM((KB, NZ, SUB, 256), BF16),
            pltpu.VMEM((2, BLK, NZ, SUB, KW), BF16),
            pltpu.VMEM((NZ, 2, 64, TC), BF16),
            pltpu.VMEM((BLK, NZ, SUB, 256), BF16),
            pltpu.VMEM((BLK, NZ, SUB, 256), BF16),
            pltpu.VMEM((UNITS, 256), BF16),
            pltpu.VMEM((UNITS, 256), F32),
            pltpu.VMEM((2, UNITS, 128), BF16),
            pltpu.VMEM((UNITS // 2, 128), BF16),
            pltpu.VMEM((UNITS // 2, 128), BF16),
            pltpu.VMEM((NX * NX, 256, 128), BF16),
            pltpu.VMEM((NX * NX, 256, 128), F32),
            pltpu.VMEM((128, 128), BF16),
            pltpu.VMEM((NZ, 8, 128), F32),
            dma((2,)), dma, dma,
            dma((2,)), dma((NZ,)),
            dma((2,)), dma((2, NZ)), dma((2,)),
            dma((2,)), dma((NZ, 2)), dma((2,)), dma((NZ,)),
            dma((2, 2, 2)), dma((2, NZ, 2)),
            dma((2, 2)), dma((2, NZ, 2)),
            dma((2, 2)), dma((2, NZ)),
            dma((2,)), dma((2, NZ)), dma((2,)), dma((2,)), dma((2,)), dma((2, NZ)),
            dma((4,)), dma((9,)), dma, dma,
            dma((2,)), dma((2,)),
            dma((4,)), dma, dma((2,)),
            dma, dma,
            dma((3,)), dma,
        ],
        compiler_params=pltpu.CompilerParams(collective_id=0, has_side_effects=True, vmem_limit_bytes=60 * 1024 * 1024),
        name="dcn",
    )(
        features,
        cross_weight.transpose(0, 1, 3, 2, 4),
        cross_bias.transpose(1, 0, 2),
        tower_weight.transpose(1, 0, 2),
        tower_bias.reshape(1, 64),
        query_weight,
        candidates,
        user_vec,
        positive.reshape(NZ, 128),
    )
    return out, loss.reshape(1024)


def solution(mesh):
    torus = Mesh(
        mesh.devices.reshape(4, 4, mesh.shape["field"], mesh.shape["dim"]),
        ("batch_0", "batch_1", "field", "dim"),
    )
    in_specs = (
        P("field", "dim", BATCH),
        P(None, "field", "dim", None, None),
        P(None, "field", "dim"),
        P(("field", "dim"), None, None),
        P(("field", "dim")),
        P(("field", "dim"), None),
        P(BATCH, None),
        P(BATCH, None),
        P(BATCH),
    )
    out_specs = (P("field", "dim", BATCH), P(BATCH))
    return jax.shard_map(body, mesh=torus, in_specs=in_specs, out_specs=out_specs, check_vma=False)
```

```python
import functools
import math

import jax
import jax.numpy as jnp
from jax import lax
from jax.experimental import pallas as pl
from jax.experimental.pallas import tpu as pltpu
from jax.sharding import Mesh
from jax.sharding import PartitionSpec as P

BATCH = ("batch_0", "batch_1")
MESH = pl.DeviceIdType.MESH
F32 = jnp.float32
BF16 = jnp.bfloat16

FIELDS = 26
NX = 4
NZ = 8
HALF = 13
SUB = 16
BLK = 7
NY = 6
NREST = FIELDS + 1 - NX * NY
KB = FIELDS + 1
KA = NY * 128
KR = NREST * 128
KW = KB * 128
GROUP = 2
TC = BLK * 128 + 256
UNITS = 1024


def copy(src, dst, send, recv, where):
    return pltpu.make_async_remote_copy(
        src_ref=src, dst_ref=dst, send_sem=send, recv_sem=recv, device_id=where, device_id_type=MESH
    )


def arrived(ref, sem):
    pltpu.make_async_copy(ref, ref, sem).wait()


def slot_shift(s):
    return jnp.where(s % 2 == 1, (s + 1) // 2, (NZ - s // 2) % NZ)


def kernel(
    feat, c_w, c_b, t_w, t_b, q_w, c_own, user, target,
    out, loss_out,
    a1, a2, w, t, cur1, cur2, part, mine, rs, hop, summed, cands, logits, u_own, loss,
    w_l, t_l, u_l,
    a2a_s, a2a_r, ag1_s, ag1_r, ag1_ls, ag2_s, ag2_r, ag2_ls, ag2_lr,
    z_s, z_r, y_s, y_r, l_s, l_r, da_s, da_r, db_s, db_r, dy_s, dy_r,
    t_s, t_r, td_s, td_r, c_s, c_r, rs_s, rs_r, hop_r, o_s, o_r, g_s, g_r,
):
    x = lax.axis_index("batch_1")
    y = lax.axis_index("batch_0")
    z = lax.axis_index("dim")
    c = lax.axis_index("field")
    p = x % 2
    wide = x // 2
    tall = 1 - wide
    xr, xl = (x + 1) % NX, (x + NX - 1) % NX
    yr, yl = (y + 1) % NX, (y + NX - 1) % NX
    zr, zl = (z + 1) % NZ, (z + NZ - 1) % NZ
    first = 2 * (1 - c)

    def lanes(j):
        return pl.ds(pl.multiple_of(j * 128, 128), 128)

    def ycols(who):
        return pl.ds(pl.multiple_of(who * KA, 128), KA)

    rest = pl.ds(NX * NY * 128, KR)

    barrier = pltpu.get_barrier_semaphore()

    def greet(where):
        pl.semaphore_signal(barrier, inc=1, device_id=where, device_id_type=MESH)

    for step in range(1, NX):
        for core in range(2):
            greet({"batch_1": (x + step) % NX, "field": core})
        greet({"batch_0": (y + step) % NX})
    for step in range(1, NZ):
        for core in range(2):
            greet({"dim": (z + step) % NZ, "field": core})
    greet({"field": 1 - c})

    base = HALF * wide + 6 * p
    own_w = [(level, k) for level in range(2) for k in range(NY + NREST - 1)]

    def own_copy(level, k):
        field = NY * y + k if k < NY else NX * NY + k - NY
        return pltpu.make_async_copy(
            c_w.at[level, pl.ds(6 * p, BLK), field], w.at[level, :, z, :, lanes(field)], w_l.at[level]
        )

    @pl.when(c == wide)
    def _():
        for level, k in own_w:
            own_copy(level, k).start()

    t_copies = [
        pltpu.make_async_copy(t_w.at[base + k], t.at[z, c, :, pl.ds(128 * k, 128)], t_l)
        for k in range(BLK)
    ]
    for cp in t_copies:
        cp.start()

    u_copy = pltpu.make_async_copy(user.at[pl.ds(pl.multiple_of(128 * z, 128), 128)], u_own, u_l)

    @pl.when(c == tall)
    def _():
        u_copy.start()

    row = lax.broadcasted_iota(jnp.int32, (NZ, SUB, 256), 0) * SUB + lax.broadcasted_iota(
        jnp.int32, (NZ, SUB, 256), 1
    )
    ones = jnp.where(row < 3, 1.0, 0.0).astype(BF16)
    a1[FIELDS] = ones
    a2[FIELDS] = ones

    def bias_block(values):
        n = values.shape[1]
        eye = lax.broadcasted_iota(jnp.int32, (n, n), 0) == lax.broadcasted_iota(jnp.int32, (n, n), 1)
        col = jnp.sum(jnp.where(eye, values, 0.0), axis=1, keepdims=True)
        hi = col.astype(BF16).astype(F32)
        mid = (col - hi).astype(BF16).astype(F32)
        low = (col - hi) - mid
        lane = lax.broadcasted_iota(jnp.int32, (n, 128), 1)
        terms = jnp.where(lane == 0, hi, jnp.where(lane == 1, mid, jnp.where(lane == 2, low, 0.0)))
        return terms.astype(BF16)

    t[z, c, :, BLK * 128 : BLK * 128 + 128] = q_w[...]
    t[z, c, :, BLK * 128 + 128 :] = bias_block(t_b[...])

    @pl.when(c == wide)
    def _():
        @pl.loop(0, BLK)
        def _(f):
            for level in range(2):
                w[level, f, z, :, FIELDS * 128 :] = bias_block(c_b[6 * p + f, level : level + 1])

        for level in range(2):
            arrived(w.at[level, :, z, :, pl.ds(0, 128 * (NY + NREST - 1))], w_l.at[level])

    @pl.when(c == tall)
    def _():
        a1[pl.ds(HALF * c, HALF), z, :, lanes(p)] = feat[:, :, lanes(z)]
        cands[NX * y + x] = c_own[...]

    arrived(t.at[z, c, :, pl.ds(0, 128 * BLK)], t_l)
    lane64 = lax.broadcasted_iota(jnp.int32, (64, 128), 1)
    edge = lanes((BLK - 1) * (1 - p))
    kept = (lane64 < 64) == (p == 0)
    t[z, c, :, edge] = jnp.where(kept, t[z, c, :, edge].astype(F32), 0.0).astype(BF16)

    pl.semaphore_wait(barrier, 3 * NX - 3 + 2 * NZ - 2 + 1)

    def examples_out(low, high):
        @pl.loop(low, high)
        def _(s):
            to = (z + slot_shift(s)) % NZ
            copy(
                feat.at[:, :, lanes(to)],
                a1.at[pl.ds(HALF * c, HALF), z, :, lanes(p)],
                a2a_s.at[0], a2a_r.at[slot_shift(s)], {"dim": to, "field": tall},
            ).start()

    def along_z(ref, level, s, k, d):
        to = jnp.where(d == 0, zr, zl)
        nxt = jnp.where(s == 0, 1 + d, jnp.minimum(s + 2, NZ - 1))
        copy(ref, ref, z_s.at[level, d, k], z_r.at[level, nxt, k], {"dim": to}).start()

    def hand_over(level, s):
        ref = w.at[level, :, (z + NZ - slot_shift(s)) % NZ, :, ycols(y)]
        copy(ref, ref, da_s.at[level], da_r.at[level, s], {"field": 1 - c}).start()

    def from_z(level, s, k):
        src = (z + NZ - slot_shift(s)) % NZ
        ref = w.at[level, :, src, :, rest] if k else w.at[level, :, src, :, ycols(y)]
        onward = ((s < 5) | (s == 6)) if k else (s < 6)

        @pl.when(s > 0)
        def _():
            arrived(ref, z_r.at[level, s, k])

        @pl.when((s > 0) & onward)
        def _():
            along_z(ref, level, s, k, jnp.where(s % 2 == 1, 0, 1))

        @pl.when(s == 0)
        def _():
            along_z(ref, level, s, k, 0)
            along_z(ref, level, s, k, 1)

        if k:
            copy(ref, ref, db_s.at[level], db_r.at[level], {"field": 1 - c}).start()
        elif level == 0:
            hand_over(level, s)
        else:
            @pl.when(s > 0)
            def _():
                hand_over(level, s)

    def from_a(level, s):
        from_z(level, s, 0)

    def from_b(level, s):
        from_z(level, s, 1)

    def to_y(level, s):
        src = (z + NZ - slot_shift(s)) % NZ
        own = w.at[level, :, src, :, ycols(y)]
        arrived(own, da_r.at[level, s])
        copy(own, own, y_s.at[level, 0], y_r.at[level, s, 0], {"batch_0": yr}).start()
        copy(own, own, y_s.at[level, 1], y_r.at[level, s, 1], {"batch_0": yl}).start()

    def from_y(level, s):
        src = (z + NZ - slot_shift(s)) % NZ
        left = w.at[level, :, src, :, ycols(yl)]
        right = w.at[level, :, src, :, ycols(yr)]
        up = w.at[level, pl.ds(0, 4), src, :, ycols(yl)]
        down = w.at[level, pl.ds(4, 3), src, :, ycols(yr)]
        arrived(left, y_r.at[level, s, 0])
        copy(up, up, l_s.at[level, 0], l_r.at[level, s], {"batch_0": yr}).start()
        copy(left, left, dy_s.at[level], dy_r.at[level, s], {"field": 1 - c}).start()
        arrived(right, y_r.at[level, s, 1])
        copy(down, down, l_s.at[level, 1], l_r.at[level, s], {"batch_0": yl}).start()
        copy(right, right, dy_s.at[level], dy_r.at[level, s], {"field": 1 - c}).start()

    def to_core(level, s):
        src = (z + NZ - slot_shift(s)) % NZ
        far = (y + 2) % NX
        piece = w.at[level, :, src, :, ycols(far)]
        arrived(piece, l_r.at[level, s])
        copy(piece, piece, dy_s.at[level], dy_r.at[level, s], {"field": 1 - c}).start()

    def tower_step(s):
        src = (z + NZ - slot_shift(s)) % NZ
        whole = t.at[src, c]

        @pl.when(s == 0)
        def _():
            copy(whole, whole, t_s.at[0], t_r.at[1], {"dim": zr}).start()
            copy(whole, whole, t_s.at[1], t_r.at[2], {"dim": zl}).start()

        @pl.when((s > 0) & (s < 7))
        def _():
            arrived(whole, t_r.at[s])

        for par, to in ((1, zr), (0, zl)):
            d = 1 - par
            half = t.at[src, c, pl.ds(32 * d, 32)]

            @pl.when((s > 0) & (s < 5) & (s % 2 == par))
            def _():
                copy(whole, whole, t_s.at[d], t_r.at[s + 2], {"dim": to}).start()

            @pl.when(s == 6 - par)
            def _():
                copy(half, half, t_s.at[2 + d], t_r.at[7 + d], {"dim": to}).start()

        @pl.when(s == 7)
        def _():
            arrived(t.at[src, c, pl.ds(0, 32)], t_r.at[7])
            arrived(t.at[src, c, pl.ds(32, 32)], t_r.at[8])

        copy(whole, whole, td_s, td_r, {"field": 1 - c}).start()

    def example_step(s):
        dz = slot_shift(s)
        src = (z + NZ - dz) % NZ
        whole = a1.at[pl.ds(0, FIELDS), src, :, lanes(p)]

        @pl.when(s == 0)
        def _():
            arrived(a1.at[pl.ds(0, HALF), src, :, lanes(p)], a2a_r.at[0])

        @pl.when(s > 0)
        def _():
            arrived(whole, a2a_r.at[dz])

        copy(whole, whole, ag1_s.at[0], ag1_r.at[p, s], {"batch_1": xr}).start()
        copy(whole, whole, ag1_s.at[1], ag1_r.at[p, s], {"batch_1": xl}).start()

    def relay_step(s):
        src = (z + NZ - slot_shift(s)) % NZ
        for j in range(2):
            r = (x + NX - first - j) % NX
            whole = a1.at[pl.ds(0, FIELDS), src, :, pl.ds(128 * j, 128)]

            @pl.when(r == 1)
            def _():
                arrived(whole, ag1_r.at[j, s])
                half = a1.at[pl.ds(0, HALF), src, :, pl.ds(128 * j, 128)]
                copy(half, half, ag1_ls.at[0], ag1_r.at[j, s], {"batch_1": xr}).start()

            @pl.when(r == 3)
            def _():
                arrived(whole, ag1_r.at[j, s])
                half = a1.at[pl.ds(HALF, HALF), src, :, pl.ds(128 * j, 128)]
                copy(half, half, ag1_ls.at[1], ag1_r.at[j, s], {"batch_1": xl}).start()

    def far_step(s):
        src = (z + NZ - slot_shift(s)) % NZ
        for j in range(2):
            r = (x + NX - first - j) % NX

            @pl.when(r == 2)
            def _():
                arrived(a1.at[pl.ds(0, FIELDS), src, :, pl.ds(128 * j, 128)], ag1_r.at[j, s])

    def owned(who, src, act):
        whole = src // 4 == who % 2

        @pl.when(whole)
        def _():
            act(HALF * (who // 2) + 6 * (who % 2), 7)

        @pl.when(jnp.logical_not(whole))
        def _():
            act(HALF * (who // 2) + 7 * (who % 2), 6)

    def second_send(s):
        src = (z + NZ - slot_shift(s)) % NZ

        def act(field, n):
            mineh = cur1.at[pl.ds(field - base, n), src]
            there = a2.at[pl.ds(field, n), src]
            copy(mineh, there, ag2_s.at[0], ag2_r.at[s, 0], {"batch_1": xr}).start()
            copy(mineh, there, ag2_s.at[1], ag2_r.at[s, 1], {"batch_1": xl}).start()
            there[...] = mineh[...]

        owned(x, src, act)

    def second_step(s):
        src = (z + NZ - slot_shift(s)) % NZ
        for d, who, to in ((0, xl, xr), (1, xr, xl)):
            def act(field, n):
                piece = a2.at[pl.ds(field, n), src]
                arrived(piece, ag2_r.at[s, d])

                @pl.when(src % 2 == 1 - d)
                def _():
                    copy(piece, piece, ag2_ls.at[d], ag2_lr.at[s], {"batch_1": to}).start()

            owned(who, src, act)

    def second_far(s):
        src = (z + NZ - slot_shift(s)) % NZ

        def act(field, n):
            arrived(a2.at[pl.ds(field, n), src], ag2_lr.at[s])

        owned((x + 2) % NX, src, act)

    def crossed(to, j):
        def act(field, n):
            copy(
                cur2.at[pl.ds(field - base, n), to, :, lanes(j)],
                out.at[pl.ds(field - HALF * wide, n), :, lanes(z)],
                o_s, o_r, {"batch_1": first + j, "dim": to, "field": wide},
            ).start()

        owned(x, to, act)

    def crossed_away(to):
        @pl.when(c == wide)
        def _():
            crossed(to, 0)
            crossed(to, 1)

        @pl.when(c == tall)
        def _():
            crossed(to, 1 - p)

    def layer(level, group):
        srcs = [(z + NZ - slot_shift(GROUP * group + g)) % NZ for g in range(GROUP)]
        rows = BLK * SUB

        def stacked(ref):
            return jnp.concatenate([ref(src).reshape(rows, -1) for src in srcs], axis=0)

        rhs = (a2 if level else a1)[...].reshape(KW, 256)
        prod = jnp.dot(stacked(lambda src: w[level, :, src]), rhs, preferred_element_type=F32)
        for g, src in enumerate(srcs):
            anchor = a1[pl.ds(base, BLK), src].reshape(rows, 256).astype(F32)
            before = cur1[:, src].reshape(rows, 256).astype(F32) if level else anchor
            nxt = (anchor * prod[g * rows : (g + 1) * rows] + before).astype(BF16).reshape(BLK, SUB, 256)
            if level:
                cur2[:, src] = nxt
            else:
                cur1[:, src] = nxt

        for g, src in enumerate(srcs):
            if level:
                @pl.when(c == tall)
                def _():
                    crossed(src, p)

                @pl.when(GROUP * group < 4)
                def _():
                    crossed_away(src)
            else:
                second_send(GROUP * group + g)

    def rows_here(level, s):
        src = (z + NZ - slot_shift(s)) % NZ

        @pl.when(c == wide)
        def _():
            arrived(w.at[level, :, src, :, pl.ds(0, 3 * KA)], dy_r.at[level, s])

    def each(low, high, step):
        @pl.loop(low, high)
        def _(s):
            step(s)

    def at(i, plan, step):
        for due, low, high in plan:
            @pl.when(i == due)
            def _():
                each(low, high, step)

    def layers(level, low, high):
        @pl.loop(low // GROUP, high // GROUP)
        def _(k):
            for g in range(GROUP):
                rows_here(level, GROUP * k + g)
            layer(level, k)

    @pl.when(c == wide)
    def _():
        from_a(0, 0)
        copy(
            feat.at[:, :, lanes(z)],
            a1.at[pl.ds(HALF * c, HALF), z, :, lanes(p)],
            a2a_s.at[1], a2a_r.at[0], {"field": tall},
        ).start()
        hand_over(1, 0)
        examples_out(1, 3)

        @pl.loop(1, 13)
        def _(i):
            @pl.when(i < NZ)
            def _():
                from_a(0, i)

            for due, low, high in ((2, 3, 5), (4, 5, 7), (5, 7, 8)):
                @pl.when(i == due)
                def _():
                    examples_out(low, high)

            @pl.when((i >= 2) & (i < 10))
            def _():
                from_b(0, i - 2)

            @pl.when(i >= 6)
            def _():
                from_a(1, i - 6)

            at(i, ((5, 0, 1), (6, 1, 2), (7, 2, 4), (8, 4, 7), (9, 7, 8)), relay_step)

            @pl.when(i == 8)
            def _():
                tower_step(0)

            @pl.when(i == 7)
            def _():
                from_b(1, 0)

            @pl.when(i == 11)
            def _():
                tower_step(1)
                tower_step(2)

            @pl.when(i == 10)
            def _():
                each(1, 3, functools.partial(from_b, 1))
                each(0, NZ, far_step)
                layers(0, 0, 4)

        layers(0, 4, NZ)
        each(3, 5, functools.partial(from_b, 1))
        from_a(1, 7)

    @pl.when(c == tall)
    def _():
        examples_out(1, 3)
        to_y(0, 0)
        to_y(1, 0)
        for step in range(1, NX):
            to = (x + step) % NX
            copy(
                c_own, cands.at[NX * y + x], c_s.at[0], c_r.at[0], {"batch_1": to, "field": 1 - to // 2}
            ).start()
        example_step(0)
        from_y(0, 0)

        @pl.loop(1, 11)
        def _(i):
            @pl.when(i < NZ)
            def _():
                to_y(0, i)

            for due in (1, 2, 3):
                @pl.when(i == due)
                def _():
                    examples_out(2 * due + 1, min(2 * due + 3, NZ))

            @pl.when(i == 1)
            def _():
                from_y(1, 0)

            @pl.when((i > 1) & (i < NZ + 1))
            def _():
                from_y(0, i - 1)

            at(i, ((2, 1, 2), (3, 2, 3), (4, 3, 5), (5, 5, 7), (6, 7, 8)), example_step)

            @pl.when(i >= 8)
            def _():
                to_y(1, i - 7)

            @pl.when(i >= 3)
            def _():
                to_core(0, i - 3)

            at(i, ((3, 0, 1), (4, 1, 2), (5, 2, 3), (6, 3, 5), (7, 5, 7), (8, 7, 8)), relay_step)

            @pl.when(i == 4)
            def _():
                to_core(1, 0)

            @pl.when(i == 5)
            def _():
                tower_step(0)

            @pl.when(i == 9)
            def _():
                tower_step(1)
                tower_step(2)
                arrived(w.at[0, :, :, :, rest], db_r.at[0])
                layers(0, 0, 4)

        to_y(1, 4)
        layers(0, 4, NZ)

    @pl.when(c == wide)
    def _():
        each(0, 4, second_step)
        each(3, 5, tower_step)
        each(4, NZ, second_step)
        each(5, 7, functools.partial(from_b, 1))
        each(5, 7, tower_step)
        from_b(1, 7)

    @pl.when(c == tall)
    def _():
        @pl.loop(1, NZ)
        def _(i):
            from_y(1, i)

            @pl.when(i < 4)
            def _():
                to_y(1, i + 4)

            for due, low, high in ((2, 3, 5), (5, 5, 7), (7, 7, 8)):
                @pl.when(i == due)
                def _():
                    each(low, high, tower_step)

            @pl.when(i < 5)
            def _():
                each(2 * i - 2, 2 * i, second_step)

            @pl.when(i >= 4)
            def _():
                to_core(1, i - 3)

        to_core(1, 5)
        arrived(w.at[1, :, :, :, rest], db_r.at[1])

    @pl.loop(0, NZ)
    def _(s):
        second_far(s)

    layers(1, 0, 4)

    @pl.when(c == wide)
    def _():
        tower_step(7)

    @pl.when(c == tall)
    def _():
        to_core(1, 6)
        to_core(1, 7)
        got = cands.at[pl.ds(NX * y, NX)]
        arrived(cands.at[pl.ds(NX * y, NX - 1)], c_r.at[0])
        for step in range(1, NX):
            copy(got, got, c_s.at[1], c_r.at[1], {"batch_0": (y + step) % NX}).start()

    layers(1, 4, NZ)

    arrived(t.at[:, c], td_r)

    def tower(k):
        lhs = t[pl.ds(2 * k, 2), :, :, 0 : BLK * 128].reshape(256, BLK * 128)
        prod = jnp.dot(lhs, cur2[...].reshape(BLK * 128, 256), preferred_element_type=F32)
        part[pl.ds(256 * k, 256)] = prod.astype(BF16)
        mine[pl.ds(256 * k, 256)] = prod

    def far_sum(k):
        for j in range(2):
            @pl.when((x + NX - first - j) % NX == 2)
            def _():
                copy(
                    part.at[pl.ds(256 * k, 256), pl.ds(128 * j, 128)],
                    hop.at[pl.ds(256 * (k % 2), 256)],
                    rs_s.at[k // 2], hop_r.at[k % 2], {"batch_1": (xr, xl)[k // 2]},
                ).start()

    for k in range(4):
        tower(k)
        far_sum(k)

    for r, own, added, way in ((1, 0, 512, xl), (3, 512, 0, xr)):
        for j in range(2):
            @pl.when((x + NX - first - j) % NX == r)
            def _():
                cols = pl.ds(128 * j, 128)
                slot = rs.at[r // 2]
                copy(
                    part.at[pl.ds(own, 512), cols], slot.at[pl.ds(own, 512)], rs_s.at[2], rs_r, {"batch_1": way}
                ).start()
                for q in range(2):
                    here, there = pl.ds(256 * q, 256), pl.ds(added + 256 * q, 256)
                    arrived(hop.at[here], hop_r.at[q])
                    summed[here] = (mine[there, cols] + hop[here].astype(F32)).astype(BF16)
                    copy(summed.at[here], slot.at[there], rs_s.at[3], rs_r, {"batch_1": way}).start()

    each(4, NZ, lambda s: crossed_away((z + NZ - slot_shift(s)) % NZ))

    @pl.when(c == tall)
    def _():
        arrived(rs, rs_r)

    for j in range(2):
        r = (x + NX - first - j) % NX

        @pl.when(r == 2)
        def _():
            arrived(hop, rs_s.at[0])
            arrived(hop, rs_s.at[1])

        @pl.when((r == 1) | (r == 3))
        def _():
            arrived(hop, rs_s.at[2])
            arrived(hop, rs_s.at[3])

    @pl.when(c == tall)
    def _():
        here = lanes(p)
        bias = t[:, :, :, BLK * 128 + 128 :].reshape(UNITS, 128).astype(F32)
        bias = bias[:, 0:1] + bias[:, 1:2] + bias[:, 2:3]
        total = mine[:, here] + rs[0].astype(F32) + rs[1].astype(F32)
        hidden = jnp.maximum(total + bias, 0.0).astype(BF16)
        qw = t[:, :, :, BLK * 128 : BLK * 128 + 128].reshape(UNITS, 128)
        query = lax.dot_general(qw, hidden, (((0,), (0,)), ((), ())), preferred_element_type=F32)
        u_copy.wait()
        query = (query + u_own[...].astype(F32).T).astype(BF16)

        arrived(cands.at[pl.ds(0, 3 * NX)], c_r.at[1])
        scale = 1.0 / math.sqrt(128)

        def scores(k, top):
            got = jnp.dot(cands[k], query, preferred_element_type=F32) * scale
            logits[k] = got
            return jnp.maximum(top, jnp.max(got.reshape(32, 8, 128), axis=0))

        top = lax.fori_loop(0, NX * NX, scores, jnp.full((8, 128), -1e30, F32), unroll=4)
        top = jnp.max(top, axis=0, keepdims=True)
        wanted = target[pl.ds(z, 1), :]
        index = lax.broadcasted_iota(jnp.int32, (256, 128), 0)

        def fold(k, carry):
            total, picked = carry
            got = logits[k]
            e = jnp.exp(got - top)
            hit = jnp.where(index == wanted - 256 * k, got, 0.0)
            return (
                total + jnp.sum(e.reshape(32, 8, 128), axis=0),
                picked + jnp.sum(hit.reshape(32, 8, 128), axis=0),
            )

        zero = jnp.zeros((8, 128), F32)
        total, picked = lax.fori_loop(0, NX * NX, fold, (zero, zero), unroll=4)
        total = jnp.sum(total, axis=0, keepdims=True)
        picked = jnp.sum(picked, axis=0, keepdims=True)
        result = top + jnp.log(total) - picked
        loss[z] = jnp.broadcast_to(result, (8, 128))

        @pl.loop(1, NZ)
        def _(dz):
            to = (z + dz) % NZ
            copy(loss.at[z], loss.at[z], g_s.at[0], g_r, {"dim": to}).start()
            copy(loss.at[z], loss.at[z], g_s.at[1], g_r, {"dim": to, "field": wide}).start()

        copy(loss.at[z], loss.at[z], g_s.at[2], g_r, {"field": wide}).start()
        arrived(loss.at[pl.ds(0, NZ - 1)], g_r)
        arrived(loss.at[pl.ds(0, NZ - 1)], g_s.at[0])
        arrived(loss.at[pl.ds(0, NZ - 1)], g_s.at[1])
        arrived(loss.at[0], g_s.at[2])
        arrived(cands.at[pl.ds(0, 3)], c_s.at[0])
        arrived(cands.at[pl.ds(0, 3 * NX)], c_s.at[1])
        for d in range(2):
            arrived(a1.at[pl.ds(0, FIELDS), :, :, pl.ds(0, 128)], ag1_s.at[d])
        for level in range(2):
            for d in range(2):
                arrived(w.at[level, :, :, :, pl.ds(0, KA)], y_s.at[level, d])
            arrived(w.at[level, pl.ds(0, 4), :, :, pl.ds(0, KA)], l_s.at[level, 0])
            arrived(w.at[level, pl.ds(4, 3), :, :, pl.ds(0, KA)], l_s.at[level, 1])
            arrived(w.at[level, :, :, :, pl.ds(0, 3 * KA)], dy_s.at[level])

    @pl.when(c == wide)
    def _():
        arrived(loss, g_r)
        arrived(feat.at[:, :, pl.ds(0, 128)], a2a_s.at[1])
        for level in range(2):
            arrived(w.at[level, :, pl.ds(0, 4), :, pl.ds(0, KA)], z_s.at[level, 0, 0])
            arrived(w.at[level, :, pl.ds(0, 3), :, pl.ds(0, KA)], z_s.at[level, 1, 0])
            arrived(w.at[level, :, pl.ds(0, 3), :, rest], z_s.at[level, 0, 1])
            arrived(w.at[level, :, pl.ds(0, 4), :, rest], z_s.at[level, 1, 1])
            arrived(w.at[level, :, :, :, pl.ds(0, KA)], da_s.at[level])
            arrived(w.at[level, :, :, :, rest], db_s.at[level])

    arrived(feat.at[:, :, pl.ds(0, 128 * (NZ - 1))], a2a_s.at[0])
    for j in range(2):
        r = (x + NX - first - j) % NX

        @pl.when(r == 1)
        def _():
            arrived(a1.at[pl.ds(0, HALF), :, :, pl.ds(0, 128)], ag1_ls.at[0])

        @pl.when(r == 3)
        def _():
            arrived(a1.at[pl.ds(0, HALF), :, :, pl.ds(0, 128)], ag1_ls.at[1])

    for d in range(2):
        arrived(a2.at[pl.ds(0, HALF), pl.ds(0, 4)], ag2_s.at[d])
        arrived(a2.at[pl.ds(0, HALF), pl.ds(0, 2)], ag2_ls.at[d])
    for d in range(2):
        arrived(t.at[pl.ds(0, 3), 0], t_s.at[d])
        arrived(t.at[0, 0, pl.ds(0, 32)], t_s.at[2 + d])
    arrived(t.at[:, 0], td_s)
    arrived(a1.at[pl.ds(0, HALF), :, :, pl.ds(0, 128)], o_s)
    for k in range(NZ):
        loss_out[k : k + 1] = loss[k, 0:1]
    arrived(out, o_r)


def body(features, cross_weight, cross_bias, tower_weight, tower_bias, query_weight, user_vec, candidates, positive):
    vmem = pl.BlockSpec(memory_space=pltpu.VMEM)
    hbm = pl.BlockSpec(memory_space=pl.ANY)
    dma = pltpu.SemaphoreType.DMA
    out, loss = pl.pallas_call(
        kernel,
        out_shape=(
            pltpu.VMEM((HALF, SUB, 1024), BF16),
            pltpu.VMEM((NZ, 128), F32),
        ),
        in_specs=[vmem, hbm, vmem, hbm, vmem, vmem, vmem, hbm, vmem],
        out_specs=(vmem, vmem),
        scratch_shapes=[
            pltpu.VMEM((KB, NZ, SUB, 256), BF16),
            pltpu.VMEM((KB, NZ, SUB, 256), BF16),
            pltpu.VMEM((2, BLK, NZ, SUB, KW), BF16),
            pltpu.VMEM((NZ, 2, 64, TC), BF16),
            pltpu.VMEM((BLK, NZ, SUB, 256), BF16),
            pltpu.VMEM((BLK, NZ, SUB, 256), BF16),
            pltpu.VMEM((UNITS, 256), BF16),
            pltpu.VMEM((UNITS, 256), F32),
            pltpu.VMEM((2, UNITS, 128), BF16),
            pltpu.VMEM((UNITS // 2, 128), BF16),
            pltpu.VMEM((UNITS // 2, 128), BF16),
            pltpu.VMEM((NX * NX, 256, 128), BF16),
            pltpu.VMEM((NX * NX, 256, 128), F32),
            pltpu.VMEM((128, 128), BF16),
            pltpu.VMEM((NZ, 8, 128), F32),
            dma((2,)), dma, dma,
            dma((2,)), dma((NZ,)),
            dma((2,)), dma((2, NZ)), dma((2,)),
            dma((2,)), dma((NZ, 2)), dma((2,)), dma((NZ,)),
            dma((2, 2, 2)), dma((2, NZ, 2)),
            dma((2, 2)), dma((2, NZ, 2)),
            dma((2, 2)), dma((2, NZ)),
            dma((2,)), dma((2, NZ)), dma((2,)), dma((2,)), dma((2,)), dma((2, NZ)),
            dma((4,)), dma((9,)), dma, dma,
            dma((2,)), dma((2,)),
            dma((4,)), dma, dma((2,)),
            dma, dma,
            dma((3,)), dma,
        ],
        compiler_params=pltpu.CompilerParams(collective_id=0, has_side_effects=True, vmem_limit_bytes=60 * 1024 * 1024),
        name="dcn",
    )(
        features,
        cross_weight.transpose(0, 1, 3, 2, 4),
        cross_bias.transpose(1, 0, 2),
        tower_weight.transpose(1, 0, 2),
        tower_bias.reshape(1, 64),
        query_weight,
        candidates,
        user_vec,
        positive.reshape(NZ, 128),
    )
    return out, loss.reshape(1024)


def solution(mesh):
    torus = Mesh(
        mesh.devices.reshape(4, 4, mesh.shape["field"], mesh.shape["dim"]),
        ("batch_0", "batch_1", "field", "dim"),
    )
    in_specs = (
        P("field", "dim", BATCH),
        P(None, "field", "dim", None, None),
        P(None, "field", "dim"),
        P(("field", "dim"), None, None),
        P(("field", "dim")),
        P(("field", "dim"), None),
        P(BATCH, None),
        P(BATCH, None),
        P(BATCH),
    )
    out_specs = (P("field", "dim", BATCH), P(BATCH))
    return jax.shard_map(body, mesh=torus, in_specs=in_specs, out_specs=out_specs, check_vma=False)
```
